32 devices in a mesh: ey: 8 (over z, y), ex: 4 (over x, core).
Axes of the slice: x: 2, y: 2, z: 4, core: 2. Of those that a mesh axis runs over, the one named last changes fastest.
Arguments:
- x: bfloat16 [512, 2048], P(('ey', 'ex'))
- kv_k: bfloat16 [512, 256, 4, 128], P(('ey', 'ex'))
- kv_v: bfloat16 [512, 256, 4, 128], P(('ey', 'ex'))
- lens: int32 [512], P(('ey', 'ex'))
- topk_idx: int32 [512, 8], P(('ey', 'ex'))
- gates: float32 [512, 8], P(('ey', 'ex'))
- ln1: bfloat16 [2048], replicated
- ln2: bfloat16 [2048], replicated
- wq: bfloat16 [2048, 4096], replicated
- wo: bfloat16 [4096, 2048], replicated
- ws1: bfloat16 [2048, 768], replicated
- ws3: bfloat16 [2048, 768], replicated
- ws2: bfloat16 [768, 2048], replicated
- w1: bfloat16 [128, 2048, 768], P(('ey', 'ex'))
- w3: bfloat16 [128, 2048, 768], P(('ey', 'ex'))
- w2: bfloat16 [128, 768, 2048], P(('ey', 'ex'))
Outputs:
- output: bfloat16 [512, 2048], P(('ey', 'ex'))
All inputs are finite; a program needn't handle non-finite values.
Results may differ from the reference program's by a relative error of at most 0.0121136.
Values are sent between devices in bfloat16 or wider.
A program may use at most 1 GiB of HBM per device.

```python
import jax
import jax.numpy as jnp
from jax import lax

EY = 8
EX = 4
TOKENS = 16
LEN = 256
D = 2048
HEADS = 32
KV_HEADS = 4
HEAD = 128
FF = 768
EXPERTS = 128
TOP = 8
ROWS_MAX = 2
CAP = 4
EPS = 1e-6
GATE_SCALE = 2.5

NDEV = EY * EX
NT = NDEV * TOKENS
EROW = EXPERTS // EY
NSLOT = EXPERTS * NDEV * CAP


def _normal(key, shape, scale):
    return (scale * jax.random.normal(key, shape, jnp.float32)).astype(jnp.bfloat16)


def _stack(key, n, shape, scale):
    return lax.map(lambda k: _normal(k, shape, scale), jax.random.split(key, n))


def _route(key):
    place_key, token_key = jax.random.split(key)
    places = jax.random.permutation(place_key, jnp.arange(EXPERTS, dtype=jnp.int32))
    half_count = EXPERTS // 2
    upper_span = EXPERTS - 1 - half_count
    offset = places - half_count
    square = offset * offset
    weight = jnp.where(offset < 0, 100 - (square * 78) // (half_count * half_count), 100 + (square * 350) // (upper_span * upper_span)).astype(jnp.uint32)
    row_of = jnp.arange(EXPERTS) // EROW

    def pick_one(one_key):
        order_key, count_key, noise_key = jax.random.split(one_key, 3)
        row_order = jax.random.permutation(order_key, EY)
        rows_used = jax.random.randint(count_key, (), 1, ROWS_MAX + 1)
        allowed = jnp.zeros((EY,), jnp.int32).at[row_order].set((jnp.arange(EY) < rows_used).astype(jnp.int32))
        noise_bits = jax.random.bits(noise_key, (EXPERTS,), jnp.uint32) >> 10
        waiting = jnp.where(allowed[row_of] > 0, noise_bits * weight, jnp.uint32(0xFFFFFFFF))
        return jnp.argsort(waiting)[:TOP]
    return jax.vmap(pick_one)(jax.random.split(token_key, NT)).astype(jnp.int32)


def setup_inputs(seed: int = 0) -> dict:
    ks = jax.random.split(jax.random.key(seed), 16)
    kd = jax.random.split(jax.random.fold_in(jax.random.key(seed), 7), 3)
    hd = HEADS * HEAD
    full = jax.random.uniform(kd[0], (NT,), jnp.float32) < 0.3
    short = jax.random.randint(kd[1], (NT,), 1, LEN // 8 + 1, jnp.int32)
    return {
        'x': _normal(ks[0], (NT, D), 1.0),
        'kv_k': _stack(ks[1], NT, (LEN, KV_HEADS, HEAD), 2.0),
        'kv_v': _stack(ks[2], NT, (LEN, KV_HEADS, HEAD), 1.0),
        'lens': jnp.where(full, LEN, short).astype(jnp.int32),
        'topk_idx': _route(kd[2]),
        'gates': GATE_SCALE * jax.nn.softmax(0.5 * jax.random.normal(ks[5], (NT, TOP), jnp.float32), axis=-1),
        'ln1': (1.0 + 0.1 * jax.random.normal(ks[6], (D,), jnp.float32)).astype(jnp.bfloat16),
        'ln2': (1.0 + 0.1 * jax.random.normal(ks[7], (D,), jnp.float32)).astype(jnp.bfloat16),
        'wq': _normal(ks[8], (D, hd), D ** -0.5),
        'wo': _normal(ks[9], (hd, D), hd ** -0.5),
        'ws1': _normal(ks[10], (D, FF), D ** -0.5),
        'ws3': _normal(ks[11], (D, FF), D ** -0.5),
        'ws2': _normal(ks[12], (FF, D), FF ** -0.5),
        'w1': _stack(ks[13], EXPERTS, (D, FF), D ** -0.5),
        'w3': _stack(ks[14], EXPERTS, (D, FF), D ** -0.5),
        'w2': _stack(ks[15], EXPERTS, (FF, D), FF ** -0.5),
    }


def _rms(v, w):
    v = v.astype(jnp.float32)
    r = lax.rsqrt(jnp.mean(v * v, axis=-1, keepdims=True) + EPS)
    return (v * r * w.astype(jnp.float32)).astype(jnp.bfloat16)


def _ffn(u, w1, w3, w2):
    g = jnp.dot(u, w1, preferred_element_type=jnp.float32)
    v = jnp.dot(u, w3, preferred_element_type=jnp.float32)
    z = (jax.nn.silu(g) * v).astype(jnp.bfloat16)
    return jnp.dot(z, w2, preferred_element_type=jnp.float32).astype(jnp.bfloat16)


def _attn(x, kk, vv, lens, ln1, wq, wo):
    b = x.shape[0]
    a = _rms(x, ln1)
    q = jnp.dot(a, wq, preferred_element_type=jnp.float32).astype(jnp.bfloat16)
    q = q.reshape(b, KV_HEADS, HEADS // KV_HEADS, HEAD).astype(jnp.float32)
    s = jnp.einsum('bkgd,blkd->bkgl', q, kk.astype(jnp.float32)) * HEAD ** -0.5
    valid = jnp.arange(LEN)[None, :] < lens[:, None]
    s = jnp.where(valid[:, None, None, :], s, -jnp.inf)
    p = jax.nn.softmax(s, axis=-1).astype(jnp.bfloat16).astype(jnp.float32)
    o = jnp.einsum('bkgl,blkd->bkgd', p, vv.astype(jnp.float32)).astype(jnp.bfloat16)
    attn = jnp.dot(o.reshape(b, HEADS * HEAD), wo, preferred_element_type=jnp.float32)
    return (x.astype(jnp.float32) + attn).astype(jnp.bfloat16)


def _slots(topk_idx, gates):
    chosen = (topk_idx[:, :, None] == jnp.arange(EXPERTS)[None, None, :]).any(axis=1).astype(jnp.int32)
    chosen = chosen.reshape(NDEV, TOKENS, EXPERTS)
    before = (jnp.cumsum(chosen, axis=1) - chosen).reshape(NT, EXPERTS)
    rank = jnp.take_along_axis(before, topk_idx, axis=1)
    src = (jnp.arange(NT, dtype=jnp.int32) // TOKENS)[:, None]
    pos = jnp.where(rank < CAP, (topk_idx * NDEV + src) * CAP + rank, NSLOT).reshape(-1)
    tok = jnp.broadcast_to(jnp.arange(NT, dtype=jnp.int32)[:, None], (NT, TOP)).reshape(-1)
    slot_tok = jnp.full((NSLOT,), NT, jnp.int32).at[pos].set(tok, mode='drop')
    slot_gate = jnp.zeros((NSLOT,), jnp.float32).at[pos].set(gates.reshape(-1), mode='drop')
    return slot_tok.reshape(EXPERTS, NDEV * CAP), slot_gate.reshape(EXPERTS, NDEV * CAP)


def reference(x, kv_k, kv_v, lens, topk_idx, gates, ln1, ln2, wq, wo, ws1, ws3, ws2, w1, w3, w2):
    per_dev = lambda a: a.reshape((NDEV, TOKENS) + a.shape[1:])
    h = lax.map(lambda t: _attn(t[0], t[1], t[2], t[3], ln1, wq, wo),
                (per_dev(x), per_dev(kv_k), per_dev(kv_v), per_dev(lens))).reshape(NT, D)
    u = _rms(h, ln2)
    slot_tok, slot_gate = _slots(topk_idx, gates)
    u_pad = jnp.concatenate([u, jnp.zeros((1, D), jnp.bfloat16)], axis=0)

    def expert(acc, xs):
        tok, gate, a1, a3, a2 = xs
        e = _ffn(u_pad[tok], a1, a3, a2)
        return acc.at[tok].add(gate[:, None] * e.astype(jnp.float32)), None

    routed, _ = lax.scan(expert, jnp.zeros((NT + 1, D), jnp.float32), (slot_tok, slot_gate, w1, w3, w2))
    y = h.astype(jnp.float32) + _ffn(u, ws1, ws3, ws2).astype(jnp.float32) + routed[:NT]
    return y.astype(jnp.bfloat16)
```

```python
import functools

import jax
import jax.numpy as jnp
from jax import lax
from jax.experimental import pallas as pl
from jax.experimental.pallas import tpu as pltpu
from jax.sharding import PartitionSpec as P

EPS = 1e-6
BF = jnp.bfloat16
F32 = jnp.float32
I32 = jnp.int32

D = 2048
FF = 768
NT = 512
CAPE = 4
NC = 4
CW = D // NC
MW = 128


def _rms(v, w):
    v = v.astype(F32)
    r = lax.rsqrt(jnp.mean(v * v, axis=-1, keepdims=True) + EPS)
    return (v * r * w.astype(F32)).astype(BF)


def _attn(x, kk, vv, lens, ln1, wq, wo):
    b, l, kvh, dh = kk.shape
    hq = wq.shape[1] // dh
    a = _rms(x, ln1)
    q = jnp.dot(a, wq, preferred_element_type=F32).astype(BF).reshape(b, kvh, hq // kvh, dh)
    s = jnp.einsum('bkgd,blkd->bkgl', q, kk, preferred_element_type=F32) * dh ** -0.5
    valid = jnp.arange(l)[None, :] < lens[:, None]
    s = jnp.where(valid[:, None, None, :], s, -jnp.inf)
    p = jax.nn.softmax(s, axis=-1).astype(BF)
    o = jnp.einsum('bkgl,blkd->bkgd', p, vv, preferred_element_type=F32).astype(BF)
    attn = jnp.dot(o.reshape(b, hq * dh), wo, preferred_element_type=F32)
    return (x.astype(F32) + attn).astype(BF)


def _split3(v):
    a = v.astype(BF)
    r = v - a.astype(F32)
    b = r.astype(BF)
    c = (r - b.astype(F32)).astype(BF)
    return a, b, c


def _dot(a, b):
    return jnp.dot(a, b, preferred_element_type=F32)


def _dot_tt(a, b):
    return lax.dot_general(a, b, (((1,), (1,)), ((), ())), preferred_element_type=F32)


def _dot_00(a, b):
    return lax.dot_general(a, b, (((0,), (0,)), ((), ())), preferred_element_type=F32)


def _moe_kernel(cap, ue_ref, h_ref, ws1, ws3, ws2, w1, w3, w2, out_ref,
                u0, u1, u2, u3, wa, wb, wc, xe, zz, fc, gm, lmat,
                ps, ra, rx, ry, dz_buf, rz, base,
                wsem, ags, agr, cbs, cbr):
    us = (u0, u1, u2, u3)
    iy = lax.axis_index('ey')
    ix = lax.axis_index('ex')
    z, y = iy // 2, iy % 2
    x, k = ix // 2, ix % 2
    dev = iy * 4 + ix

    def zdev(d):
        return (((z + d) % 4) * 2 + y, ix)
    ydev = (z * 2 + (1 - y), ix)
    xdev = (iy, (1 - x) * 2 + k)
    kdev = (iy, x * 2 + (1 - k))

    barrier = pltpu.get_barrier_semaphore()
    for d in (zdev(1), zdev(2), zdev(3), ydev, xdev, kdev):
        pl.semaphore_signal(barrier, inc=1, device_id=d, device_id_type=pl.DeviceIdType.MESH)

    def wcopies(slot, a, b, c, i):
        return [pltpu.make_async_copy(a, wa.at[slot], wsem.at[i, 0]),
                pltpu.make_async_copy(b, wb.at[slot], wsem.at[i, 1]),
                pltpu.make_async_copy(c, wc.at[slot], wsem.at[i, 2])]
    shared_cp = wcopies(0, ws1, ws3, ws2, 4)
    exp_cp = [wcopies((e + 1) % 4, w1.at[e], w3.at[e], w2.at[e], e) for e in range(4)]
    for cp in shared_cp:
        cp.start()
    for e in range(3):
        for cp in exp_cp[e]:
            cp.start()

    pl.semaphore_wait(barrier, 6)

    def rcopy(src, dst, s, r, d):
        return pltpu.make_async_remote_copy(src_ref=src, dst_ref=dst, send_sem=s, recv_sem=r,
                                            device_id=d, device_id_type=pl.DeviceIdType.MESH)

    offs = [0] + [MW + CW * c for c in range(1, NC)]
    wid = [MW + CW] + [CW] * (NC - 1)
    zc = []
    for c in range(NC):
        src = ue_ref.at[:, pl.ds(offs[c], wid[c])]
        cps = [rcopy(src, us[c].at[z, y, x, k], ags.at[c, d - 1], agr.at[c, d - 1], zdev(d)) for d in (1, 2, 3)]
        for cp in cps:
            cp.start()
        zc.append(cps)
        us[c][z, y, x, k] = ue_ref[:, offs[c]:offs[c] + wid[c]]

    for cp in shared_cp[:2]:
        cp.wait()
    u = ue_ref[:, MW:]
    g = _dot(u, wa[0])
    v = _dot(u, wb[0])
    zs = (jax.nn.silu(g) * v).astype(BF)
    shared_cp[2].wait()
    base[...] = h_ref[...].astype(F32) + _dot(zs, wc[0]).astype(BF).astype(F32)
    for cp in exp_cp[3]:
        cp.start()

    p1 = []
    for c in range(NC):
        for cp in zc[c]:
            cp.wait_recv()
        blk = us[c].at[:, y, x, k]
        cp = rcopy(blk, blk, ags.at[c, 3], agr.at[c, 3], ydev if c % 2 == 0 else xdev)
        cp.start()
        p1.append(cp)
    p2 = []
    for c in range(NC):
        p1[c].wait_recv()
        blk = us[c].at[:, :, x, k] if c % 2 == 0 else us[c].at[:, y, :, k]
        cp = rcopy(blk, blk, ags.at[c, 4], agr.at[c, 4], xdev if c % 2 == 0 else ydev)
        cp.start()
        p2.append(cp)
    p3 = []
    for c in range(NC):
        p2[c].wait_recv()
        blk = us[c].at[:, :, :, k]
        cp = rcopy(blk, blk, ags.at[c, 5], agr.at[c, 5], kdev)
        cp.start()
        p3.append(cp)
    p3[0].wait_recv()

    mt = u0[...].reshape(NT, MW + CW)[:, :MW].astype(F32).T
    tk = mt[0:8]
    gts = (mt[8:16], mt[16:24], mt[24:32])
    t1 = lax.broadcasted_iota(I32, (1, NT), 1)
    blk1 = t1 // 16
    ti = lax.broadcasted_iota(I32, (NT, NT), 0)
    tj = lax.broadcasted_iota(I32, (NT, NT), 1)
    earlier = ti < tj
    lmat[...] = jnp.where(earlier & (ti // 16 == tj // 16), 1.0, 0.0).astype(BF)
    ms, gs = [], []
    for e in range(4):
        eq = tk == (dev * 4 + e).astype(F32)
        ms.append(jnp.sum(jnp.where(eq, 1.0, 0.0), axis=0, keepdims=True))
        gs.append([jnp.sum(jnp.where(eq, gg, 0.0), axis=0, keepdims=True) for gg in gts])
    mstack = jnp.concatenate(ms + [jnp.zeros((4, NT), F32)], axis=0)
    before = _dot(mstack.astype(BF), lmat[...])
    slot = jnp.where((mstack > 0.5) & (before < CAPE - 0.5), (blk1 * CAPE).astype(F32) + before, -1.0)

    lmat[...] = jnp.where(earlier & ((ti // 16) % 8 == (tj // 16) % 8), 1.0, 0.0).astype(BF)

    def rowmatch(r):
        lo = (r * 16).astype(F32)
        return jnp.max(jnp.where((tk >= lo) & (tk < lo + 16.0), 1.0, 0.0), axis=0, keepdims=True)
    rm = jnp.concatenate([rowmatch(iy), rowmatch(z * 2 + (1 - y)), jnp.zeros((6, NT), F32)], axis=0)
    rb = _dot(rm.astype(BF), lmat[...])
    ridx = jnp.where((rm > 0.5) & (rb < cap - 0.5), rb, -1.0)
    gidx = ((blk1 % 2) * 2 + (blk1 // 2) % 2) * 2 + (blk1 // 4) % 2
    cidx = jnp.where(ridx[0:1] > -0.5, (gidx * cap).astype(F32) + ridx[0:1], -1.0)
    cmat = (lax.broadcasted_iota(I32, (8 * cap, NT), 0).astype(F32) == cidx).astype(F32).astype(BF)
    mine = gidx == (k * 2 + x) * 2 + y
    ci = lax.broadcasted_iota(I32, (cap, NT), 0).astype(F32)
    own = jnp.concatenate([(ci == jnp.where(mine, ridx[0:1], -1.0)).astype(F32),
                           (ci == jnp.where(mine, ridx[1:2], -1.0)).astype(F32)], axis=0).astype(BF)
    sj = lax.broadcasted_iota(I32, (NT, 64), 1)
    st = lax.broadcasted_iota(I32, (NT, 64), 0)
    sel = (st == (sj // 16) * 128 + y * 64 + ix * 16 + sj % 16).astype(F32).astype(BF)
    emat = _dot(own, sel).astype(BF)

    si = lax.broadcasted_iota(I32, (128, NT), 0).astype(F32)
    for e in range(4):
        hit = si == slot[e:e + 1]
        pe = hit.astype(F32).astype(BF)
        for m in range(3):
            gp = jnp.where(hit, gs[e][m], 0.0).astype(BF)
            gm[m, :, 128 * e:128 * (e + 1)] = _dot_tt(cmat, gp).astype(BF)
        xe[e, :, :NT] = pe

    for c in range(1, NC):
        p3[c].wait_recv()
    for e in range(4):
        pe = xe[e, :, :NT]
        for c in range(NC):
            off = MW if c == 0 else 0
            uc = us[c][...].reshape(NT, wid[c])[:, off:]
            fc[0:128, :] = _dot(pe, uc).astype(BF)
            if c > 0:
                xe[e, :, c * CW:(c + 1) * CW] = fc[0:128, :]
            else:
                fc[128:256, :] = fc[0:128, :]
        xe[e, :, :CW] = fc[128:256, :]
    for e in range(4):
        s_ = (e + 1) % 4
        exp_cp[e][0].wait()
        g = _dot(xe[e], wa[s_])
        exp_cp[e][1].wait()
        v = _dot(xe[e], wb[s_])
        zz[e] = (jax.nn.silu(g) * v).astype(BF)
    for e in range(4):
        exp_cp[e][2].wait()

    sent = []
    ca, cx, cy, cz = {}, {}, {}, {}

    def stage0(c):
        for e in range(4):
            fc[128 * e:128 * (e + 1), :] = _dot(zz[e], wc[(e + 1) % 4, :, c * CW:(c + 1) * CW]).astype(BF)
        f = fc[...]
        o = _dot(gm[0], f) + _dot(gm[1], f) + _dot(gm[2], f)
        ps[c] = o.reshape(2, 2, 2, cap, CW)
        cp = rcopy(ps.at[c, 1 - k], ra.at[c], cbs.at[c, 0], cbr.at[c, 0], kdev)
        cp.start()
        ca[c] = cp

    def stage1(c):
        ca[c].wait_recv()
        ps[c, k] = ps[c, k] + ra[c]
        cp = rcopy(ps.at[c, k, 1 - x], rx.at[c], cbs.at[c, 1], cbr.at[c, 1], xdev)
        cp.start()
        cx[c] = cp

    def stage2(c):
        cx[c].wait_recv()
        ps[c, k, x] = ps[c, k, x] + rx[c]
        cp = rcopy(ps.at[c, k, x, 1 - y], ry.at[c], cbs.at[c, 2], cbr.at[c, 2], ydev)
        cp.start()
        cy[c] = cp

    def stage3(c):
        cy[c].wait_recv()
        data = jnp.concatenate([ps[c, k, x, y], ry[c]], axis=0)
        a, b, d = _split3(data)
        dn = _dot_00(emat, a) + _dot_00(emat, b) + _dot_00(emat, d)
        dz_buf[c] = dn.reshape(4, 16, CW)
        cps = [rcopy(dz_buf.at[c, (z + d) % 4], rz.at[c, d - 1], cbs.at[c, 2 + d], cbr.at[c, 2 + d], zdev(d)) for d in (1, 2, 3)]
        for cp in cps:
            cp.start()
        cz[c] = cps

    def stage4(c):
        for cp in cz[c]:
            cp.wait_recv()
        o = base[:, c * CW:(c + 1) * CW] + dz_buf[c, z] + rz[c, 0] + rz[c, 1] + rz[c, 2]
        out_ref[:, c * CW:(c + 1) * CW] = o.astype(BF)

    stages = (stage0, stage1, stage2, stage3, stage4)
    for step in range(NC + 4):
        for s_, fn in enumerate(stages):
            c = step - s_
            if 0 <= c < NC:
                fn(c)
    for c in range(NC):
        for cp in zc[c] + [p1[c], p2[c], p3[c], ca[c], cx[c], cy[c]] + cz[c]:
            cp.wait_send()


def _moe(cap, cid, ue, h, ws1, ws3, ws2, w1, w3, w2):
    vm = pl.BlockSpec(memory_space=pltpu.VMEM)
    hb = pl.BlockSpec(memory_space=pl.ANY)
    widths = [MW + CW] + [CW] * (NC - 1)
    scratch = [pltpu.VMEM((4, 2, 2, 2, 16, w), BF) for w in widths] + [
        pltpu.VMEM((4, D, FF), BF), pltpu.VMEM((4, D, FF), BF), pltpu.VMEM((4, FF, D), BF),
        pltpu.VMEM((4, 128, D), BF), pltpu.VMEM((4, 128, FF), BF), pltpu.VMEM((512, CW), BF),
        pltpu.VMEM((3, 8 * cap, 512), BF), pltpu.VMEM((NT, NT), BF),
        pltpu.VMEM((NC, 2, 2, 2, cap, CW), F32), pltpu.VMEM((NC, 2, 2, cap, CW), F32),
        pltpu.VMEM((NC, 2, cap, CW), F32), pltpu.VMEM((NC, cap, CW), F32),
        pltpu.VMEM((NC, 4, 16, CW), F32), pltpu.VMEM((NC, 3, 16, CW), F32),
        pltpu.VMEM((16, D), F32),
        pltpu.SemaphoreType.DMA((5, 3)), pltpu.SemaphoreType.DMA((NC, 6)), pltpu.SemaphoreType.DMA((NC, 6)),
        pltpu.SemaphoreType.DMA((NC, 6)), pltpu.SemaphoreType.DMA((NC, 6)),
    ]
    return pl.pallas_call(
        functools.partial(_moe_kernel, cap),
        out_shape=jax.ShapeDtypeStruct((16, D), BF),
        in_specs=[vm, vm] + [hb] * 6,
        out_specs=vm,
        scratch_shapes=scratch,
        name='moe',
        compiler_params=pltpu.CompilerParams(collective_id=cid, has_side_effects=True, vmem_limit_bytes=66_000_000),
    )(ue, h, ws1, ws3, ws2, w1, w3, w2)


def solution(mesh):
    rows = P(('ey', 'ex'))
    rep = P()

    def local(x, kv_k, kv_v, lens, topk_idx, gates, ln1, ln2, wq, wo, ws1, ws3, ws2, w1, w3, w2):
        h = _attn(x, kv_k, kv_v, lens, ln1, wq, wo)
        u = _rms(h, ln2)
        g1 = lax.reduce_precision(gates, 8, 7)
        r = gates - g1
        g2 = lax.reduce_precision(r, 8, 7)
        g3 = r - g2
        meta = jnp.concatenate([topk_idx.astype(F32), g1, g2, g3, jnp.zeros((16, MW - 32), F32)], axis=1).astype(BF)
        ue = jnp.concatenate([meta, u], axis=1)
        return _moe(64, 1, ue, h, ws1, ws3, ws2, w1, w3, w2)

    return jax.shard_map(
        local, mesh=mesh,
        in_specs=(rows, rows, rows, rows, rows, rows, rep, rep, rep, rep, rep, rep, rep, rows, rows, rows),
        out_specs=rows, check_vma=False)
```

```python
import functools

import jax
import jax.numpy as jnp
from jax import lax
from jax.experimental import pallas as pl
from jax.experimental.pallas import tpu as pltpu
from jax.sharding import PartitionSpec as P

EPS = 1e-6
BF = jnp.bfloat16
F32 = jnp.float32
I32 = jnp.int32

D = 2048
FF = 768
NT = 512
CAPE = 4
NC = 4
CW = D // NC
MW = 128


def _rms(v, w):
    v = v.astype(F32)
    r = lax.rsqrt(jnp.mean(v * v, axis=-1, keepdims=True) + EPS)
    return (v * r * w.astype(F32)).astype(BF)


def _split3(v):
    a = v.astype(BF)
    r = v - a.astype(F32)
    b = r.astype(BF)
    c = (r - b.astype(F32)).astype(BF)
    return a, b, c


def _dot(a, b):
    return jnp.dot(a, b, preferred_element_type=F32)


def _dot_tt(a, b):
    return lax.dot_general(a, b, (((1,), (1,)), ((), ())), preferred_element_type=F32)


def _dot_00(a, b):
    return lax.dot_general(a, b, (((0,), (0,)), ((), ())), preferred_element_type=F32)


def _rcopy(src, dst, s, r, d):
    return pltpu.make_async_remote_copy(src_ref=src, dst_ref=dst, send_sem=s, recv_sem=r,
                                        device_id=d, device_id_type=pl.DeviceIdType.MESH)


class _Pos:
    def __init__(self):
        self.iy = iy = lax.axis_index('ey')
        self.ix = ix = lax.axis_index('ex')
        self.z, self.y = iy // 2, iy % 2
        self.x, self.k = ix // 2, ix % 2
        self.ydev = (self.z * 2 + (1 - self.y), ix)
        self.xdev = (iy, (1 - self.x) * 2 + self.k)
        self.kdev = (iy, self.x * 2 + (1 - self.k))

    def zdev(self, d):
        return (((self.z + d) % 4) * 2 + self.y, self.ix)

    def greet(self):
        barrier = pltpu.get_barrier_semaphore()
        for d in (self.zdev(1), self.zdev(2), self.zdev(3), self.ydev, self.xdev, self.kdev):
            pl.semaphore_signal(barrier, inc=1, device_id=d, device_id_type=pl.DeviceIdType.MESH)
        return barrier


QC = 8
OC = 4


def _attn_kernel(cap, x_ref, meta_ref, lens_ref, ln1_ref, ln2_ref, wq, wo, kk, vv,
                 h_ref, u_ref, mt_ref, flag_ref,
                 wqb, wob, kb, vb, qs, os_, mall,
                 qsem, osem, ksem, vsem, ags, agr):
    p = _Pos()
    z, y, x, k = p.z, p.y, p.x, p.k
    barrier = p.greet()

    def qcp(c):
        return pltpu.make_async_copy(wq.at[:, pl.ds(pl.multiple_of(c * 512, 512), 512)], wqb.at[c], qsem.at[c])

    def ocp(c):
        return pltpu.make_async_copy(wo.at[:, pl.ds(pl.multiple_of(c * 512, 512), 512)], wob.at[c], osem.at[c])

    def kcp(t):
        return pltpu.make_async_copy(kk.at[pl.ds(t * 4, 4)], kb.at[pl.ds(t * 4, 4)], ksem.at[t])

    def vcp(t):
        return pltpu.make_async_copy(vv.at[pl.ds(t * 4, 4)], vb.at[pl.ds(t * 4, 4)], vsem.at[t])

    for c in range(QC):
        qcp(c).start()
    for t in range(4):
        kcp(t).start()
        vcp(t).start()
    for c in range(OC):
        ocp(c).start()

    mall[z, y, x, k] = meta_ref[...]
    a = _rms(x_ref[...], ln1_ref[...])
    pl.semaphore_wait(barrier, 6)
    zc = [_rcopy(meta_ref, mall.at[z, y, x, k], ags.at[d - 1], agr.at[d - 1], p.zdev(d)) for d in (1, 2, 3)]
    for cp in zc:
        cp.start()

    def qstep(c, _):
        qcp(c).wait()
        q = _dot(a, wqb[c]).astype(BF).astype(F32)
        for j in range(4):
            qs[pl.ds(pl.multiple_of(c * 64 + j * 16, 16), 16), :] = q[:, j * 128:(j + 1) * 128]
        return 0
    lax.fori_loop(0, QC, qstep, 0)

    for cp in zc:
        cp.wait_recv()
    yb = mall.at[:, y, x, k]
    yc = _rcopy(yb, yb, ags.at[3], agr.at[3], p.ydev)
    yc.start()
    xb = mall.at[:, :, x, k]
    xc = _rcopy(xb, xb, ags.at[4], agr.at[4], p.xdev)
    kb_ = mall.at[:, :, :, k]
    kc = _rcopy(kb_, kb_, ags.at[5], agr.at[5], p.kdev)

    col = lax.broadcasted_iota(I32, (32, 1024), 1)
    row = lax.broadcasted_iota(I32, (32, 1024), 0)
    headok = (col % 4) == (row // 8)
    pos = jnp.where(headok, col // 4, 1 << 20)

    def astep(g, _):
        kcp(g).wait()
        vcp(g).wait()
        for j in range(4):
            t = g * 4 + j
            q = qs[pl.ds(t, 32, stride=16), :].astype(BF)
            s = _dot_tt(q, kb[t]) * 128.0 ** -0.5
            s = jnp.where(pos < lens_ref[t], s, -jnp.inf)
            m = jnp.max(s, axis=1, keepdims=True)
            e = jnp.exp(s - m)
            pr = (e / jnp.sum(e, axis=1, keepdims=True)).astype(BF)
            o = _dot(pr, vb[t])
            os_[pl.ds(t, 32, stride=16), :] = o

        @pl.when(g == 1)
        def _():
            yc.wait_recv()
            xc.start()

        @pl.when(g == 3)
        def _():
            xc.wait_recv()
            kc.start()
        return 0
    lax.fori_loop(0, 4, astep, 0)

    oo = jnp.concatenate([os_[h * 16:(h + 1) * 16, :] for h in range(32)], axis=1).astype(BF)

    def ostep(c, _):
        ocp(c).wait()
        sl = pl.ds(pl.multiple_of(c * 512, 512), 512)
        h_ref[:, sl] = (x_ref[:, sl].astype(F32) + _dot(oo, wob[c])).astype(BF)
        return 0
    lax.fori_loop(0, OC, ostep, 0)
    u_ref[...] = _rms(h_ref[...], ln2_ref[...])

    kc.wait_recv()
    mt = mall[...].reshape(NT, MW).astype(F32).T[0:32]
    mt_ref[...] = mt
    tk = mt[0:8]
    rm = jnp.concatenate([jnp.max(jnp.where((tk >= 16.0 * r) & (tk < 16.0 * r + 16.0), 1.0, 0.0), axis=0, keepdims=True)
                          for r in range(8)], axis=0)
    gt = (lax.broadcasted_iota(I32, (NT, 128), 0) // 16) % 8
    gsel = (gt == lax.broadcasted_iota(I32, (NT, 128), 1)).astype(F32).astype(BF)
    cnt = _dot(rm.astype(BF), gsel)
    flag_ref[...] = jnp.broadcast_to(jnp.max(cnt, axis=(0, 1), keepdims=True), (8, 128))
    for cp in zc + [yc, xc, kc]:
        cp.wait_send()


def _attn(cap, x, meta, lens, ln1, ln2, wq, wo, kk, vv):
    vm = pl.BlockSpec(memory_space=pltpu.VMEM)
    hb = pl.BlockSpec(memory_space=pl.ANY)
    return pl.pallas_call(
        functools.partial(_attn_kernel, cap),
        out_shape=(jax.ShapeDtypeStruct((16, D), BF), jax.ShapeDtypeStruct((16, D), BF),
                   jax.ShapeDtypeStruct((32, NT), F32), jax.ShapeDtypeStruct((8, 128), F32)),
        in_specs=[vm, vm, pl.BlockSpec(memory_space=pltpu.SMEM), vm, vm] + [hb] * 4,
        out_specs=(vm, vm, vm, vm),
        scratch_shapes=[
            pltpu.VMEM((QC, D, 512), BF), pltpu.VMEM((OC, 4096, 512), BF),
            pltpu.VMEM((16, 1024, 128), BF), pltpu.VMEM((16, 1024, 128), BF),
            pltpu.VMEM((512, 128), F32), pltpu.VMEM((512, 128), F32), pltpu.VMEM((4, 2, 2, 2, 16, MW), BF),
            pltpu.SemaphoreType.DMA((QC,)), pltpu.SemaphoreType.DMA((OC,)),
            pltpu.SemaphoreType.DMA((4,)), pltpu.SemaphoreType.DMA((4,)),
            pltpu.SemaphoreType.DMA((6,)), pltpu.SemaphoreType.DMA((6,)),
        ],
        name='attn',
        compiler_params=pltpu.CompilerParams(collective_id=3, has_side_effects=True, vmem_limit_bytes=60_000_000),
    )(x, meta, lens, ln1, ln2, wq, wo, kk, vv)


def _moe_kernel(cap, u_ref, h_ref, mt_ref, ws1, ws3, ws2, w1, w3, w2, out_ref,
                zb, yb, uc, wa, wb, wc, xe, zz, fc, gm, pm, lmat,
                ps, ra, rx, ry, dz_buf, rz, base,
                wsem, ags, agr, cbs, cbr):
    p = _Pos()
    iy, ix, z, y, x, k = p.iy, p.ix, p.z, p.y, p.x, p.k
    dev = iy * 4 + ix
    barrier = p.greet()

    def wcp(e, i):
        return pltpu.make_async_copy((w1, w3, w2)[i].at[e], (wa, wb, wc)[i].at[(e + 1) % 4], wsem.at[e, i])
    scp = [pltpu.make_async_copy(s, b.at[0], wsem.at[4, i]) for i, (s, b) in enumerate(((ws1, wa), (ws3, wb), (ws2, wc)))]
    for cp in scp:
        cp.start()
    for e in range(3):
        wcp(e, 0).start()
        wcp(e, 1).start()
    for e in range(3):
        wcp(e, 2).start()

    pl.semaphore_wait(barrier, 6)
    zc = []
    for c in range(NC):
        src = u_ref.at[:, pl.ds(CW * c, CW)]
        cps = [_rcopy(src, zb.at[c, z], ags.at[c, d - 1], agr.at[c, d - 1], p.zdev(d)) for d in (1, 2, 3)]
        for cp in cps:
            cp.start()
        zc.append(cps)
        zb[c, z] = u_ref[:, CW * c:CW * (c + 1)]

    tk = mt_ref[0:8]
    gts = (mt_ref[8:16], mt_ref[16:24], mt_ref[24:32])
    blk1 = lax.broadcasted_iota(I32, (1, NT), 1) // 16
    ti = lax.broadcasted_iota(I32, (NT, NT), 0)
    tj = lax.broadcasted_iota(I32, (NT, NT), 1)
    earlier = ti < tj
    lmat[...] = jnp.where(earlier & ((ti // 16) % 8 == (tj // 16) % 8), 1.0, 0.0).astype(BF)

    def rowmatch(r):
        lo = (r * 16).astype(F32)
        return jnp.max(jnp.where((tk >= lo) & (tk < lo + 16.0), 1.0, 0.0), axis=0, keepdims=True)
    rm = jnp.concatenate([rowmatch(iy), rowmatch(z * 2 + (1 - y)), jnp.zeros((6, NT), F32)], axis=0)
    rb = _dot(rm.astype(BF), lmat[...])
    ridx = jnp.where((rm > 0.5) & (rb < cap - 0.5), rb, -1.0)
    gidx = ((blk1 % 2) * 2 + (blk1 // 2) % 2) * 2 + (blk1 // 4) % 2
    mine = gidx == (k * 2 + x) * 2 + y
    ci = lax.broadcasted_iota(I32, (cap, NT), 0).astype(F32)
    own = jnp.concatenate([(ci == jnp.where(mine, ridx[0:1], -1.0)).astype(F32),
                           (ci == jnp.where(mine, ridx[1:2], -1.0)).astype(F32)], axis=0).astype(BF)
    sj = lax.broadcasted_iota(I32, (NT, 64), 1)
    st = lax.broadcasted_iota(I32, (NT, 64), 0)
    sel = (st == (sj // 16) * 128 + y * 64 + ix * 16 + sj % 16).astype(F32).astype(BF)
    emat = _dot(own, sel).astype(BF)

    yc = []
    for c in range(NC):
        for cp in zc[c]:
            cp.wait_recv()
        lst = _dot(emat, zb[c].reshape(64, CW)).astype(BF)
        yb[c] = lst[cap:]
        cp = _rcopy(yb.at[c], uc.at[c, k, x, y], ags.at[c, 3], agr.at[c, 3], p.ydev)
        cp.start()
        yc.append(cp)
        uc[c, k, x, y] = lst[:cap]

    scp[0].wait()
    scp[1].wait()
    u = u_ref[...]
    g = _dot(u, wa[0])
    v = _dot(u, wb[0])
    zs = (jax.nn.silu(g) * v).astype(BF)

    xc = []
    for c in range(NC):
        yc[c].wait_recv()
        cp = _rcopy(uc.at[c, k, x], uc.at[c, k, x], ags.at[c, 4], agr.at[c, 4], p.xdev)
        cp.start()
        xc.append(cp)

    scp[2].wait()
    base[...] = h_ref[...].astype(F32) + _dot(zs, wc[0]).astype(BF).astype(F32)
    for i in range(3):
        wcp(3, i).start()

    lmat[...] = jnp.where(earlier & (ti // 16 == tj // 16), 1.0, 0.0).astype(BF)
    ms, gs = [], []
    for e in range(4):
        eq = tk == (dev * 4 + e).astype(F32)
        ms.append(jnp.sum(jnp.where(eq, 1.0, 0.0), axis=0, keepdims=True))
        gs.append([jnp.sum(jnp.where(eq, gg, 0.0), axis=0, keepdims=True) for gg in gts])
    mstack = jnp.concatenate(ms + [jnp.zeros((4, NT), F32)], axis=0)
    before = _dot(mstack.astype(BF), lmat[...])
    slot = jnp.where((mstack > 0.5) & (before < CAPE - 0.5), (blk1 * CAPE).astype(F32) + before, -1.0)
    cidx = jnp.where(ridx[0:1] > -0.5, (gidx * cap).astype(F32) + ridx[0:1], -1.0)
    cmat = (lax.broadcasted_iota(I32, (8 * cap, NT), 0).astype(F32) == cidx).astype(F32).astype(BF)
    si = lax.broadcasted_iota(I32, (128, NT), 0).astype(F32)
    for e in range(4):
        hit = si == slot[e:e + 1]
        pm[128 * e:128 * (e + 1), :] = _dot_tt(hit.astype(F32).astype(BF), cmat).astype(BF)
        for m in range(3):
            gp = jnp.where(hit, gs[e][m], 0.0).astype(BF)
            gm[m, :, 128 * e:128 * (e + 1)] = _dot_tt(cmat, gp).astype(BF)

    kc = []
    for c in range(NC):
        xc[c].wait_recv()
        cp = _rcopy(uc.at[c, k], uc.at[c, k], ags.at[c, 5], agr.at[c, 5], p.kdev)
        cp.start()
        kc.append(cp)
    for c in range(NC):
        kc[c].wait_recv()
        xe[:, :, c * CW:(c + 1) * CW] = _dot(pm[...], uc[c].reshape(8 * cap, CW)).astype(BF).reshape(4, 128, CW)

    def ffn(e, _):
        s = (e + 1) % 4
        wcp(e, 0).wait()
        g = _dot(xe[e], wa[s])
        wcp(e, 1).wait()
        v = _dot(xe[e], wb[s])
        zz[e] = (jax.nn.silu(g) * v).astype(BF)
        return 0
    lax.fori_loop(0, 4, ffn, 0)
    for e in range(4):
        wcp(e, 2).wait()

    ca, cx, cy, cz = {}, {}, {}, {}

    def stage0(c):
        for e in range(4):
            fc[128 * e:128 * (e + 1), :] = _dot(zz[e], wc[(e + 1) % 4, :, c * CW:(c + 1) * CW]).astype(BF)
        f = fc[...]
        o = _dot(gm[0], f) + _dot(gm[1], f) + _dot(gm[2], f)
        ps[c] = o.reshape(2, 2, 2, cap, CW)
        ca[c] = _rcopy(ps.at[c, 1 - k], ra.at[c], cbs.at[c, 0], cbr.at[c, 0], p.kdev)
        ca[c].start()

    def stage1(c):
        ca[c].wait_recv()
        ps[c, k] = ps[c, k] + ra[c]
        cx[c] = _rcopy(ps.at[c, k, 1 - x], rx.at[c], cbs.at[c, 1], cbr.at[c, 1], p.xdev)
        cx[c].start()

    def stage2(c):
        cx[c].wait_recv()
        ps[c, k, x] = ps[c, k, x] + rx[c]
        cy[c] = _rcopy(ps.at[c, k, x, 1 - y], ry.at[c], cbs.at[c, 2], cbr.at[c, 2], p.ydev)
        cy[c].start()

    def stage3(c):
        cy[c].wait_recv()
        data = jnp.concatenate([ps[c, k, x, y], ry[c]], axis=0)
        a, b, d = _split3(data)
        dn = _dot_00(emat, a) + _dot_00(emat, b) + _dot_00(emat, d)
        dz_buf[c] = dn.reshape(4, 16, CW)
        cz[c] = [_rcopy(dz_buf.at[c, (z + d) % 4], rz.at[c, d - 1], cbs.at[c, 2 + d], cbr.at[c, 2 + d], p.zdev(d))
                 for d in (1, 2, 3)]
        for cp in cz[c]:
            cp.start()

    def stage4(c):
        for cp in cz[c]:
            cp.wait_recv()
        o = base[:, c * CW:(c + 1) * CW] + dz_buf[c, z] + rz[c, 0] + rz[c, 1] + rz[c, 2]
        out_ref[:, c * CW:(c + 1) * CW] = o.astype(BF)

    stages = (stage0, stage1, stage2, stage3, stage4)
    for step in range(NC + 4):
        for s, fn in enumerate(stages):
            c = step - s
            if 0 <= c < NC:
                fn(c)
    for c in range(NC):
        for cp in zc[c] + [yc[c], xc[c], kc[c], ca[c], cx[c], cy[c]] + cz[c]:
            cp.wait_send()


def _moe(cap, cid, u, h, mt, ws1, ws3, ws2, w1, w3, w2):
    vm = pl.BlockSpec(memory_space=pltpu.VMEM)
    hb = pl.BlockSpec(memory_space=pl.ANY)
    scratch = [
        pltpu.VMEM((NC, 4, 16, CW), BF), pltpu.VMEM((NC, cap, CW), BF), pltpu.VMEM((NC, 2, 2, 2, cap, CW), BF),
        pltpu.VMEM((4, D, FF), BF), pltpu.VMEM((4, D, FF), BF), pltpu.VMEM((4, FF, D), BF),
        pltpu.VMEM((4, 128, D), BF), pltpu.VMEM((4, 128, FF), BF), pltpu.VMEM((512, CW), BF),
        pltpu.VMEM((3, 8 * cap, 512), BF), pltpu.VMEM((512, 8 * cap), BF), pltpu.VMEM((NT, NT), BF),
        pltpu.VMEM((NC, 2, 2, 2, cap, CW), F32), pltpu.VMEM((NC, 2, 2, cap, CW), F32),
        pltpu.VMEM((NC, 2, cap, CW), F32), pltpu.VMEM((NC, cap, CW), F32),
        pltpu.VMEM((NC, 4, 16, CW), F32), pltpu.VMEM((NC, 3, 16, CW), F32),
        pltpu.VMEM((16, D), F32),
        pltpu.SemaphoreType.DMA((5, 3)), pltpu.SemaphoreType.DMA((NC, 6)), pltpu.SemaphoreType.DMA((NC, 6)),
        pltpu.SemaphoreType.DMA((NC, 6)), pltpu.SemaphoreType.DMA((NC, 6)),
    ]
    return pl.pallas_call(
        functools.partial(_moe_kernel, cap),
        out_shape=jax.ShapeDtypeStruct((16, D), BF),
        in_specs=[vm, vm, vm] + [hb] * 6,
        out_specs=vm,
        scratch_shapes=scratch,
        name='moe',
        compiler_params=pltpu.CompilerParams(collective_id=cid, has_side_effects=True, vmem_limit_bytes=66_000_000),
    )(u, h, mt, ws1, ws3, ws2, w1, w3, w2)


CAP = 32


def solution(mesh):
    rows = P(('ey', 'ex'))
    rep = P()

    def local(x, kv_k, kv_v, lens, topk_idx, gates, ln1, ln2, wq, wo, ws1, ws3, ws2, w1, w3, w2):
        g1 = lax.reduce_precision(gates, 8, 7)
        r = gates - g1
        g2 = lax.reduce_precision(r, 8, 7)
        g3 = r - g2
        meta = jnp.concatenate([topk_idx.astype(F32), g1, g2, g3, jnp.zeros((16, MW - 32), F32)], axis=1).astype(BF)
        h, u, mt, cnt = _attn(CAP, x, meta, lens, ln1[None], ln2[None], wq, wo,
                              kv_k.reshape(16, 1024, 128), kv_v.reshape(16, 1024, 128))
        args = (u, h, mt, ws1, ws3, ws2, w1, w3, w2)
        return lax.cond(cnt[0, 0] > CAP + 0.5, functools.partial(_moe, 64, 2), functools.partial(_moe, CAP, 1), *args)

    return jax.shard_map(
        local, mesh=mesh,
        in_specs=(rows, rows, rows, rows, rows, rows, rep, rep, rep, rep, rep, rep, rep, rows, rows, rows),
        out_specs=rows, check_vma=False)
```

```python
import functools

import jax
import jax.numpy as jnp
from jax import lax
from jax.experimental import pallas as pl
from jax.experimental.pallas import tpu as pltpu
from jax.sharding import PartitionSpec as P

EPS = 1e-6
BF = jnp.bfloat16
F32 = jnp.float32
I32 = jnp.int32

D = 2048
FF = 768
NT = 512
CAPE = 4
NC = 4
CW = D // NC
CC = 4
CX = D // CC
MW = 128


def _rms(v, w):
    v = v.astype(F32)
    r = lax.rsqrt(jnp.mean(v * v, axis=-1, keepdims=True) + EPS)
    return (v * r * w.astype(F32)).astype(BF)


def _split3(v):
    a = v.astype(BF)
    r = v - a.astype(F32)
    b = r.astype(BF)
    c = (r - b.astype(F32)).astype(BF)
    return a, b, c


def _dot(a, b):
    return jnp.dot(a, b, preferred_element_type=F32)


def _dot_tt(a, b):
    return lax.dot_general(a, b, (((1,), (1,)), ((), ())), preferred_element_type=F32)


def _dot_00(a, b):
    return lax.dot_general(a, b, (((0,), (0,)), ((), ())), preferred_element_type=F32)


def _rcopy(src, dst, s, r, d):
    return pltpu.make_async_remote_copy(src_ref=src, dst_ref=dst, send_sem=s, recv_sem=r,
                                        device_id=d, device_id_type=pl.DeviceIdType.MESH)


class _Pos:
    def __init__(self):
        self.iy = iy = lax.axis_index('ey')
        self.ix = ix = lax.axis_index('ex')
        self.z, self.y = iy // 2, iy % 2
        self.x, self.k = ix // 2, ix % 2
        self.ydev = (self.z * 2 + (1 - self.y), ix)
        self.xdev = (iy, (1 - self.x) * 2 + self.k)
        self.kdev = (iy, self.x * 2 + (1 - self.k))

    def zdev(self, d):
        return (((self.z + d) % 4) * 2 + self.y, self.ix)

    def far(self, d):
        return (((self.z + d) % 4) * 2 + 1 - self.y, self.ix)

    def greet(self):
        barrier = pltpu.get_barrier_semaphore()
        for d in self.column() + self.row():
            pl.semaphore_signal(barrier, inc=1, device_id=d, device_id_type=pl.DeviceIdType.MESH)
        return barrier

    def column(self):
        return [self.zdev(d) for d in range(1, 4)] + [self.far(d) for d in range(4)]

    def row(self):
        return [(self.iy, (self.ix + d) % 4) for d in range(1, 4)]


def _layer_kernel(cap, capc, win_ref, x_ref, topk_ref, gates_ref, lens_ref, ln1_ref, ln2_ref,
                  wq, wo, kk, vv, ws1, ws3, ws2, w1, w3, w2, out_ref, flag_ref,
                  g1b, g2b, kb, vb, qs, os_, mall, mscr, mt_ref, u_ref,
                  zb, yb, uc, xe, zz, fc, gm, pm, ps, ra, rx, ry, dz_buf, rz, base,
                  qsem, osem, ksem, vsem, esem, mgs, mgr, ags, agr, cbs, cbr):
    p = _Pos()
    iy, ix, z, y, x, k = p.iy, p.ix, p.z, p.y, p.x, p.k
    dev = iy * 4 + ix
    barrier = p.greet()

    def qcp(c):
        sl = pl.ds(pl.multiple_of(c * 512, 512), 512)
        return pltpu.make_async_copy(wq.at[:, sl], g1b.at[:, sl], qsem.at[c])

    def ocp(c):
        sl = pl.ds(pl.multiple_of(c * 512, 512), 512)
        return pltpu.make_async_copy(wo.at[sl], g2b.at[sl], osem.at[c])

    def kcp(t):
        return pltpu.make_async_copy(kk.at[pl.ds(t * 4, 4)], kb.at[pl.ds(t * 4, 4)], ksem.at[t])

    def vcp(t):
        return pltpu.make_async_copy(vv.at[pl.ds(t * 4, 4)], vb.at[pl.ds(t * 4, 4)], vsem.at[t])

    def col13(e, i):
        return pl.ds(pl.multiple_of((2 * e + i) * FF, 256), FF)

    def wcp(e, i):
        if i == 2:
            return pltpu.make_async_copy(w2.at[e], g2b.at[pl.ds(pl.multiple_of(e * FF, 256), FF)], esem.at[e, 2])
        return pltpu.make_async_copy((w1, w3)[i].at[e], g1b.at[:, col13(e, i)], esem.at[e, i])
    scp = [pltpu.make_async_copy(ws1, g1b.at[:, col13(3, 0)], esem.at[4, 0]),
           pltpu.make_async_copy(ws3, g1b.at[:, col13(3, 1)], esem.at[4, 1]),
           pltpu.make_async_copy(ws2, g2b.at[pl.ds(4 * FF, FF)], esem.at[4, 2])]

    for c in range(8):
        qcp(c).start()
    for t in range(4):
        kcp(t).start()
        vcp(t).start()
    for c in range(8):
        ocp(c).start()
    scp[0].start()
    scp[1].start()

    mscr[...] = jnp.zeros((128, 128), F32)
    mscr[0:8, 0:16] = topk_ref[...].astype(F32)
    for i, part in enumerate(_split3(gates_ref[...])):
        mscr[8 + 8 * i:16 + 8 * i, 0:16] = part.astype(F32)
    mall[z, y, x, k] = mscr[...].T[0:16].astype(BF)
    a = _rms(x_ref[...], ln1_ref[...].reshape(1, D))

    own = mall.at[z, y, x, k]
    m1 = [_rcopy(own, own, mgs.at[i], mgr.at[i], d) for i, d in enumerate(p.column())]
    col = mall.at[:, :, x, k]
    m2 = [_rcopy(col, col, mgs.at[7 + i], mgr.at[7 + i], d) for i, d in enumerate(p.row())]

    def qstep(c, _):
        @pl.when(c == 5)
        def _():
            pl.semaphore_wait(barrier, 10)
            for cp in m1:
                cp.start()
        qcp(c).wait()
        q = _dot(a, g1b[:, pl.ds(pl.multiple_of(c * 512, 512), 512)]).astype(BF).astype(F32)
        for j in range(4):
            qs[pl.ds(pl.multiple_of(c * 64 + j * 16, 16), 16), :] = q[:, j * 128:(j + 1) * 128]
        return 0
    lax.fori_loop(0, 8, qstep, 0)
    for e in range(3):
        wcp(e, 0).start()
        wcp(e, 1).start()

    col = lax.broadcasted_iota(I32, (64, 1024), 1)
    row = lax.broadcasted_iota(I32, (64, 1024), 0)
    pos = jnp.where((col % 4) == (row % 32) // 8, col // 4, 1 << 20)
    first = lax.broadcasted_iota(I32, (64, 1), 0) < 32
    nil = jnp.zeros((32, 128), BF)

    def astep(g, _):
        @pl.when(g == 2)
        def _():
            for cp in m1:
                cp.wait_recv()
            for cp in m2:
                cp.start()
        kcp(g).wait()
        vcp(g).wait()
        for j in range(2):
            t = g * 4 + 2 * j
            qa = qs[pl.ds(t, 32, stride=16), :].astype(BF)
            qb = qs[pl.ds(t + 1, 32, stride=16), :].astype(BF)
            q2 = jnp.concatenate([jnp.concatenate([qa, nil], axis=1), jnp.concatenate([nil, qb], axis=1)], axis=0)
            s = _dot_tt(q2, jnp.concatenate([kb[t], kb[t + 1]], axis=1))
            s = jnp.where(pos < jnp.where(first, lens_ref[t], lens_ref[t + 1]), s, -jnp.inf)
            m = jnp.max(s, axis=1, keepdims=True)
            e = jnp.exp((s - m) * 128.0 ** -0.5)
            pr = (e * (1.0 / jnp.sum(e, axis=1, keepdims=True))).astype(BF)
            o = _dot(pr, jnp.concatenate([vb[t], vb[t + 1]], axis=1))
            os_[pl.ds(t, 32, stride=16), :] = o[:32, :128]
            os_[pl.ds(t + 1, 32, stride=16), :] = o[32:, 128:]
        return 0
    lax.fori_loop(0, 4, astep, 0)

    base[...] = x_ref[...].astype(F32)

    def ostep(c, _):
        ocp(c).wait()
        oc = jnp.concatenate([os_[pl.ds(pl.multiple_of(c * 64 + j * 16, 16), 16), :] for j in range(4)], axis=1).astype(BF)
        base[...] += _dot(oc, g2b[pl.ds(pl.multiple_of(c * 512, 512), 512), :])
        return 0
    lax.fori_loop(0, 8, ostep, 0)
    h = base[...].astype(BF)
    u_ref[...] = _rms(h, ln2_ref[...].reshape(1, D))
    base[...] = h.astype(F32)

    zc = []
    for c in range(NC):
        zb[c, z] = u_ref[:, CW * c:CW * (c + 1)]
    for c in range(NC):
        blk = zb.at[c, z]
        cps = [_rcopy(blk, blk, ags.at[c, d - 1], agr.at[c, d - 1], p.zdev(d)) for d in (1, 2, 3)]
        for cp in cps:
            cp.start()
        zc.append(cps)
    scp[2].start()
    for e in range(4):
        wcp(e, 2).start()

    for cp in m2:
        cp.wait_recv()
    def flags():
        mt = mall[...].reshape(NT, MW).astype(F32).T[0:32]
        mt_ref[...] = mt
        tk = mt[0:8]
        rm = jnp.concatenate([jnp.max(jnp.where((tk >= 16.0 * r) & (tk < 16.0 * r + 16.0), 1.0, 0.0), axis=0, keepdims=True)
                              for r in range(8)], axis=0)
        gt = (lax.broadcasted_iota(I32, (NT, 128), 0) // 16) % 8
        gsel = (gt == lax.broadcasted_iota(I32, (NT, 128), 1)).astype(F32).astype(BF)
        cnt = _dot(rm.astype(BF), gsel)
        flag_ref[0] = jnp.max(cnt).astype(I32)

    flags()
    tk = mt_ref[0:8]
    gts = (mt_ref[8:16], mt_ref[16:24], mt_ref[24:32])
    blk1 = lax.broadcasted_iota(I32, (1, NT), 1) // 16
    ti = lax.broadcasted_iota(I32, (NT, NT), 0)
    tj = lax.broadcasted_iota(I32, (NT, NT), 1)
    earlier = ti < tj
    fc[...] = jnp.where(earlier & ((ti // 16) % 8 == (tj // 16) % 8), 1.0, 0.0).astype(BF)

    def rowmatch(r):
        lo = (r * 16).astype(F32)
        return jnp.max(jnp.where((tk >= lo) & (tk < lo + 16.0), 1.0, 0.0), axis=0, keepdims=True)
    rm = jnp.concatenate([rowmatch(iy), rowmatch(z * 2 + (1 - y)), jnp.zeros((6, NT), F32)], axis=0)
    rb = _dot(rm.astype(BF), fc[...])
    rb = rb - win_ref[0].astype(F32) * capc
    ridx = jnp.where((rm > 0.5) & (rb > -0.5) & (rb < capc - 0.5), rb, -1.0)
    gidx = ((blk1 % 2) * 2 + (blk1 // 2) % 2) * 2 + (blk1 // 4) % 2
    mine = gidx == (k * 2 + x) * 2 + y
    sj = lax.broadcasted_iota(I32, (NT, 64), 1)
    st = lax.broadcasted_iota(I32, (NT, 64), 0)
    sel = (st == (sj // 16) * 128 + y * 64 + ix * 16 + sj % 16).astype(F32).astype(BF)

    def mylist(n):
        ci = lax.broadcasted_iota(I32, (n, NT), 0).astype(F32)
        own = jnp.concatenate([(ci == jnp.where(mine, ridx[i:i + 1], -1.0)).astype(F32) for i in range(2)], axis=0)
        return _dot(own.astype(BF), sel).astype(BF)
    emat = mylist(cap)
    ematc = mylist(capc) if capc != cap else emat

    yc = []
    for c in range(NC):
        for cp in zc[c]:
            cp.wait_recv()
        lst = _dot(emat, zb[c].reshape(64, CW)).astype(BF)
        yb[c] = lst[cap:]
        cp = _rcopy(yb.at[c], uc.at[c, k, x, y], ags.at[c, 3], agr.at[c, 3], p.ydev)
        cp.start()
        yc.append(cp)
        uc[c, k, x, y] = lst[:cap]

    scp[0].wait()
    scp[1].wait()
    u = u_ref[...]
    g = _dot(u, g1b[:, 6 * FF:7 * FF])
    v = _dot(u, g1b[:, 7 * FF:8 * FF])
    zs = (jax.nn.silu(g) * v).astype(BF)
    for i in range(2):
        wcp(3, i).start()

    xc = []
    for c in range(NC):
        yc[c].wait_recv()
        cp = _rcopy(uc.at[c, k, x], uc.at[c, k, x], ags.at[c, 4], agr.at[c, 4], p.xdev)
        cp.start()
        xc.append(cp)

    scp[2].wait()
    full = base[...] + _dot(zs, g2b[4 * FF:5 * FF, :]).astype(BF).astype(F32)
    base[...] = jnp.where(win_ref[0] == 0, full, 0.0)

    fc[...] = jnp.where(earlier & (ti // 16 == tj // 16), 1.0, 0.0).astype(BF)
    ms, gs = [], []
    for e in range(4):
        eq = tk == (dev * 4 + e).astype(F32)
        ms.append(jnp.sum(jnp.where(eq, 1.0, 0.0), axis=0, keepdims=True))
        gs.append([jnp.sum(jnp.where(eq, gg, 0.0), axis=0, keepdims=True) for gg in gts])
    mstack = jnp.concatenate(ms + [jnp.zeros((4, NT), F32)], axis=0)
    before = _dot(mstack.astype(BF), fc[...])
    slot = jnp.where((mstack > 0.5) & (before < CAPE - 0.5), (blk1 * CAPE).astype(F32) + before, -1.0)
    def allists(n):
        cidx = jnp.where(ridx[0:1] > -0.5, (gidx * n).astype(F32) + ridx[0:1], -1.0)
        return (lax.broadcasted_iota(I32, (8 * n, NT), 0).astype(F32) == cidx).astype(F32).astype(BF)
    cmat = allists(cap)
    cmatc = allists(capc) if capc != cap else cmat
    si = lax.broadcasted_iota(I32, (128, NT), 0).astype(F32)
    for e in range(4):
        hit = si == slot[e:e + 1]
        pm[128 * e:128 * (e + 1), :] = _dot_tt(hit.astype(F32).astype(BF), cmat).astype(BF)
        for m in range(3):
            gp = jnp.where(hit, gs[e][m], 0.0).astype(BF)
            gm[m, :, 128 * e:128 * (e + 1)] = _dot_tt(cmatc, gp).astype(BF)

    kc = []
    for c in range(NC):
        xc[c].wait_recv()
        cp = _rcopy(uc.at[c, k], uc.at[c, k], ags.at[c, 5], agr.at[c, 5], p.kdev)
        cp.start()
        kc.append(cp)
    for c in range(NC):
        kc[c].wait_recv()
        xe[:, :, c * CW:(c + 1) * CW] = _dot(pm[...], uc[c].reshape(8 * cap, CW)).astype(BF).reshape(4, 128, CW)

    def ffn(e, _):
        wcp(e, 0).wait()
        g = _dot(xe[e], g1b[:, col13(e, 0)])
        wcp(e, 1).wait()
        v = _dot(xe[e], g1b[:, col13(e, 1)])
        zz[e] = (jax.nn.silu(g) * v).astype(BF)
        return 0
    lax.fori_loop(0, 4, ffn, 0)
    for e in range(4):
        wcp(e, 2).wait()

    ca, cx, cy, cz = {}, {}, {}, {}

    def stage0(c):
        for e in range(4):
            fc[128 * e:128 * (e + 1), :] = _dot(zz[e], g2b[FF * e:FF * (e + 1), c * CX:(c + 1) * CX]).astype(BF)
        f = fc[...]
        o = _dot(gm[0], f) + _dot(gm[1], f) + _dot(gm[2], f)
        ps[c] = o.reshape(2, 2, 2, capc, CX)
        ca[c] = _rcopy(ps.at[c, 1 - k], ra.at[c], cbs.at[c, 0], cbr.at[c, 0], p.kdev)
        ca[c].start()

    def stage1(c):
        ca[c].wait_recv()
        ps[c, k] = ps[c, k] + ra[c]
        cx[c] = _rcopy(ps.at[c, k, 1 - x], rx.at[c], cbs.at[c, 1], cbr.at[c, 1], p.xdev)
        cx[c].start()

    def stage2(c):
        cx[c].wait_recv()
        ps[c, k, x] = ps[c, k, x] + rx[c]
        cy[c] = _rcopy(ps.at[c, k, x, 1 - y], ry.at[c], cbs.at[c, 2], cbr.at[c, 2], p.ydev)
        cy[c].start()

    def stage3(c):
        cy[c].wait_recv()
        data = jnp.concatenate([ps[c, k, x, y], ry[c]], axis=0)
        a, b, d = _split3(data)
        dn = _dot_00(ematc, a) + _dot_00(ematc, b) + _dot_00(ematc, d)
        dz_buf[c] = dn.reshape(4, 16, CX)
        cz[c] = [_rcopy(dz_buf.at[c, (z + d) % 4], rz.at[c, d - 1], cbs.at[c, 2 + d], cbr.at[c, 2 + d], p.zdev(d))
                 for d in (1, 2, 3)]
        for cp in cz[c]:
            cp.start()

    def stage4(c):
        for cp in cz[c]:
            cp.wait_recv()
        o = base[:, c * CX:(c + 1) * CX] + dz_buf[c, z] + rz[c, 0] + rz[c, 1] + rz[c, 2]
        out_ref[:, c * CX:(c + 1) * CX] = o

    stages = (stage0, stage1, stage2, stage3, stage4)
    for step in range(CC + 4):
        for s, fn in enumerate(stages):
            c = step - s
            if 0 <= c < CC:
                fn(c)
    for c in range(NC):
        for cp in zc[c] + [yc[c], xc[c], kc[c]]:
            cp.wait_send()
    for cp in m1 + m2:
        cp.wait_send()
    for c in range(CC):
        for cp in [ca[c], cx[c], cy[c]] + cz[c]:
            cp.wait_send()


def _layer(cap, capc, win, x, topk, gates, lens, ln1, ln2, *big):
    vm = pl.BlockSpec(memory_space=pltpu.VMEM)
    sm = pl.BlockSpec(memory_space=pltpu.SMEM)
    hb = pl.BlockSpec(memory_space=pl.ANY)
    dma = pltpu.SemaphoreType.DMA
    scratch = [
        pltpu.VMEM((D, 8 * FF), BF), pltpu.VMEM((4096, D), BF),
        pltpu.VMEM((16, 1024, 128), BF), pltpu.VMEM((16, 1024, 128), BF),
        pltpu.VMEM((512, 128), F32), pltpu.VMEM((512, 128), F32), pltpu.VMEM((4, 2, 2, 2, 16, MW), BF),
        pltpu.VMEM((128, 128), F32), pltpu.VMEM((32, NT), F32), pltpu.VMEM((16, D), BF),
        pltpu.VMEM((NC, 4, 16, CW), BF), pltpu.VMEM((NC, cap, CW), BF), pltpu.VMEM((NC, 2, 2, 2, cap, CW), BF),
        pltpu.VMEM((4, 128, D), BF), pltpu.VMEM((4, 128, FF), BF), pltpu.VMEM((512, 512), BF),
        pltpu.VMEM((3, 8 * capc, 512), BF), pltpu.VMEM((512, 8 * cap), BF),
        pltpu.VMEM((CC, 2, 2, 2, capc, CX), F32), pltpu.VMEM((CC, 2, 2, capc, CX), F32),
        pltpu.VMEM((CC, 2, capc, CX), F32), pltpu.VMEM((CC, capc, CX), F32),
        pltpu.VMEM((CC, 4, 16, CX), F32), pltpu.VMEM((CC, 3, 16, CX), F32), pltpu.VMEM((16, D), F32),
        dma((8,)), dma((8,)), dma((4,)), dma((4,)), dma((5, 3)), dma((10,)), dma((10,)),
        dma((NC, 6)), dma((NC, 6)), dma((CC, 6)), dma((CC, 6)),
    ]
    return pl.pallas_call(
        functools.partial(_layer_kernel, cap, capc),
        out_shape=(jax.ShapeDtypeStruct((16, D), F32), jax.ShapeDtypeStruct((1,), I32)),
        in_specs=[sm, vm, vm, vm, sm, vm, vm] + [hb] * 10,
        out_specs=(vm, sm),
        scratch_shapes=scratch,
        name='layer',
        compiler_params=pltpu.CompilerParams(collective_id=1, has_side_effects=True, vmem_limit_bytes=67_043_328),
    )(jnp.full((1,), win, I32), x, topk, gates, lens, ln1, ln2, *big)


CAPD = 32
CAPC = 24


def solution(mesh):
    rows = P(('ey', 'ex'))
    rep = P()

    def local(x, kv_k, kv_v, lens, topk_idx, gates, ln1, ln2, wq, wo, ws1, ws3, ws2, w1, w3, w2):
        args = (x, topk_idx.T, gates.T, lens, ln1, ln2, wq, wo, kv_k.reshape(16, 1024, 128), kv_v.reshape(16, 1024, 128),
                ws1, ws3, ws2, w1, w3, w2)
        acc, most = _layer(CAPD, CAPC, 0, *args)

        def more(acc, args):
            for win in range(1, -(-64 // CAPC)):
                acc += _layer(CAPD, CAPC, win, *args)[0]
            return acc
        return lax.cond(most[0] > CAPC, more, lambda acc, _: acc, acc, args).astype(BF)

    return jax.shard_map(
        local, mesh=mesh,
        in_specs=(rows, rows, rows, rows, rows, rows, rep, rep, rep, rep, rep, rep, rep, rows, rows, rows),
        out_specs=rows, check_vma=False)
```

```python
import functools

import jax
import jax.numpy as jnp
from jax import lax
from jax.experimental import pallas as pl
from jax.experimental.pallas import tpu as pltpu
from jax.sharding import PartitionSpec as P

EPS = 1e-6
BF = jnp.bfloat16
F32 = jnp.float32
I32 = jnp.int32

D = 2048
FF = 768
NT = 512
CAPE = 4
NC = 4
CW = D // NC
CC = 4
CX = D // CC
MW = 128


def _rms(v, w):
    v = v.astype(F32)
    r = lax.rsqrt(jnp.mean(v * v, axis=-1, keepdims=True) + EPS)
    return (v * r * w.astype(F32)).astype(BF)


def _split3(v):
    a = v.astype(BF)
    r = v - a.astype(F32)
    b = r.astype(BF)
    c = (r - b.astype(F32)).astype(BF)
    return a, b, c


def _dot(a, b):
    return jnp.dot(a, b, preferred_element_type=F32)


def _dot_tt(a, b):
    return lax.dot_general(a, b, (((1,), (1,)), ((), ())), preferred_element_type=F32)


def _dot_00(a, b):
    return lax.dot_general(a, b, (((0,), (0,)), ((), ())), preferred_element_type=F32)


def _rcopy(src, dst, s, r, d):
    return pltpu.make_async_remote_copy(src_ref=src, dst_ref=dst, send_sem=s, recv_sem=r,
                                        device_id=d, device_id_type=pl.DeviceIdType.MESH)


class _Pos:
    def __init__(self):
        self.iy = iy = lax.axis_index('ey')
        self.ix = ix = lax.axis_index('ex')
        self.z, self.y = iy // 2, iy % 2
        self.x, self.k = ix // 2, ix % 2
        self.ydev = (self.z * 2 + (1 - self.y), ix)
        self.xdev = (iy, (1 - self.x) * 2 + self.k)
        self.kdev = (iy, self.x * 2 + (1 - self.k))

    def zdev(self, d):
        return (((self.z + d) % 4) * 2 + self.y, self.ix)

    def far(self, d):
        return (((self.z + d) % 4) * 2 + 1 - self.y, self.ix)

    def greet(self):
        barrier = pltpu.get_barrier_semaphore()
        for d in self.column() + self.row():
            pl.semaphore_signal(barrier, inc=1, device_id=d, device_id_type=pl.DeviceIdType.MESH)
        return barrier

    def column(self):
        return [self.zdev(d) for d in range(1, 4)] + [self.far(d) for d in range(4)]

    def row(self):
        return [(self.iy, (self.ix + d) % 4) for d in range(1, 4)]


def _layer_kernel(cap, capc, win_ref, lens_ref, x_hbm, topk_hbm, gates_hbm, ln1_hbm, ln2_hbm,
                  wq, wo, kk, vv, ws1, ws3, ws2, w1, w3, w2, out_ref, flag_ref,
                  x_ref, topk_ref, gates_ref, ln1_ref, ln2_ref, g1b, g2b, kb, vb, qs, os_, mall, mscr, mt_ref, u_ref,
                  zb, yb, uc, xe, zz, fc, gm, pm, ps, ra, rx, ry, dz_buf, rz, base,
                  isem, qsem, osem, ksem, vsem, esem, mgs, mgr, ags, agr, cbs, cbr):
    p = _Pos()
    iy, ix, z, y, x, k = p.iy, p.ix, p.z, p.y, p.x, p.k
    dev = iy * 4 + ix
    small = [pltpu.make_async_copy(s, d, isem.at[i]) for i, (s, d) in enumerate((
        (x_hbm, x_ref), (topk_hbm, topk_ref), (gates_hbm, gates_ref), (ln1_hbm, ln1_ref), (ln2_hbm, ln2_ref)))]
    for cp in small:
        cp.start()
    barrier = p.greet()

    def qcp(c):
        sl = pl.ds(pl.multiple_of(c * 512, 512), 512)
        return pltpu.make_async_copy(wq.at[:, sl], g1b.at[:, sl], qsem.at[c])

    def ocp(c):
        sl = pl.ds(pl.multiple_of(c * 512, 512), 512)
        return pltpu.make_async_copy(wo.at[sl], g2b.at[sl], osem.at[c])

    def kcp(t):
        return pltpu.make_async_copy(kk.at[pl.ds(t * 4, 4)], kb.at[pl.ds(t * 4, 4)], ksem.at[t])

    def vcp(t):
        return pltpu.make_async_copy(vv.at[pl.ds(t * 4, 4)], vb.at[pl.ds(t * 4, 4)], vsem.at[t])

    def col13(e, i):
        return pl.ds(pl.multiple_of((2 * e + i) * FF, 256), FF)

    def wcp(e, i):
        if i == 2:
            return pltpu.make_async_copy(w2.at[e], g2b.at[pl.ds(pl.multiple_of(e * FF, 256), FF)], esem.at[e, 2])
        return pltpu.make_async_copy((w1, w3)[i].at[e], g1b.at[:, col13(e, i)], esem.at[e, i])
    scp = [pltpu.make_async_copy(ws1, g1b.at[:, col13(3, 0)], esem.at[4, 0]),
           pltpu.make_async_copy(ws3, g1b.at[:, col13(3, 1)], esem.at[4, 1]),
           pltpu.make_async_copy(ws2, g2b.at[pl.ds(4 * FF, FF)], esem.at[4, 2])]

    for c in range(8):
        qcp(c).start()
    for t in range(4):
        kcp(t).start()
        vcp(t).start()
    for c in range(8):
        ocp(c).start()
    scp[0].start()
    scp[1].start()

    for cp in small:
        cp.wait()
    mscr[...] = jnp.zeros((128, 128), F32)
    mscr[0:8, 0:16] = topk_ref[...].astype(F32)
    for i, part in enumerate(_split3(gates_ref[...])):
        mscr[8 + 8 * i:16 + 8 * i, 0:16] = part.astype(F32)
    mall[z, y, x, k] = mscr[...].T[0:16].astype(BF)
    a = _rms(x_ref[...], ln1_ref[...].reshape(1, D))

    own = mall.at[z, y, x, k]
    m1 = [_rcopy(own, own, mgs.at[i], mgr.at[i], d) for i, d in enumerate(p.column())]
    col = mall.at[:, :, x, k]
    m2 = [_rcopy(col, col, mgs.at[7 + i], mgr.at[7 + i], d) for i, d in enumerate(p.row())]

    def qstep(c, _):
        @pl.when(c == 5)
        def _():
            pl.semaphore_wait(barrier, 10)
            for cp in m1:
                cp.start()
        qcp(c).wait()
        q = _dot(a, g1b[:, pl.ds(pl.multiple_of(c * 512, 512), 512)]).astype(BF).astype(F32)
        for j in range(4):
            qs[pl.ds(pl.multiple_of(c * 64 + j * 16, 16), 16), :] = q[:, j * 128:(j + 1) * 128]
        return 0
    lax.fori_loop(0, 8, qstep, 0)
    for e in range(3):
        wcp(e, 0).start()
        wcp(e, 1).start()

    col = lax.broadcasted_iota(I32, (64, 1024), 1)
    row = lax.broadcasted_iota(I32, (64, 1024), 0)
    pos = jnp.where((col % 4) == (row % 32) // 8, col // 4, 1 << 20)
    first = lax.broadcasted_iota(I32, (64, 1), 0) < 32
    nil = jnp.zeros((32, 128), BF)

    def astep(g, _):
        @pl.when(g == 2)
        def _():
            for cp in m1:
                cp.wait_recv()
            for cp in m2:
                cp.start()
        kcp(g).wait()
        vcp(g).wait()
        for j in range(2):
            t = g * 4 + 2 * j
            qa = qs[pl.ds(t, 32, stride=16), :].astype(BF)
            qb = qs[pl.ds(t + 1, 32, stride=16), :].astype(BF)
            q2 = jnp.concatenate([jnp.concatenate([qa, nil], axis=1), jnp.concatenate([nil, qb], axis=1)], axis=0)
            s = _dot_tt(q2, jnp.concatenate([kb[t], kb[t + 1]], axis=1))
            s = jnp.where(pos < jnp.where(first, lens_ref[t], lens_ref[t + 1]), s, -jnp.inf)
            m = jnp.max(s, axis=1, keepdims=True)
            e = jnp.exp((s - m) * 128.0 ** -0.5)
            pr = (e * (1.0 / jnp.sum(e, axis=1, keepdims=True))).astype(BF)
            o = _dot(pr, jnp.concatenate([vb[t], vb[t + 1]], axis=1))
            os_[pl.ds(t, 32, stride=16), :] = o[:32, :128]
            os_[pl.ds(t + 1, 32, stride=16), :] = o[32:, 128:]
        return 0
    lax.fori_loop(0, 4, astep, 0)

    base[...] = x_ref[...].astype(F32)

    def ostep(c, _):
        ocp(c).wait()
        oc = jnp.concatenate([os_[pl.ds(pl.multiple_of(c * 64 + j * 16, 16), 16), :] for j in range(4)], axis=1).astype(BF)
        base[...] += _dot(oc, g2b[pl.ds(pl.multiple_of(c * 512, 512), 512), :])
        return 0
    lax.fori_loop(0, 8, ostep, 0)
    h = base[...].astype(BF)
    u_ref[...] = _rms(h, ln2_ref[...].reshape(1, D))
    base[...] = h.astype(F32)

    zc = []
    for c in range(NC):
        zb[c, z] = u_ref[:, CW * c:CW * (c + 1)]
    for c in range(NC):
        blk = zb.at[c, z]
        cps = [_rcopy(blk, blk, ags.at[c, d - 1], agr.at[c, d - 1], p.zdev(d)) for d in (1, 2, 3)]
        for cp in cps:
            cp.start()
        zc.append(cps)
    scp[2].start()
    for e in range(4):
        wcp(e, 2).start()

    for cp in m2:
        cp.wait_recv()
    def flags():
        mt = mall[...].reshape(NT, MW).astype(F32).T[0:32]
        mt_ref[...] = mt
        tk = mt[0:8]
        rm = jnp.concatenate([jnp.max(jnp.where((tk >= 16.0 * r) & (tk < 16.0 * r + 16.0), 1.0, 0.0), axis=0, keepdims=True)
                              for r in range(8)], axis=0)
        gt = (lax.broadcasted_iota(I32, (NT, 128), 0) // 16) % 8
        gsel = (gt == lax.broadcasted_iota(I32, (NT, 128), 1)).astype(F32).astype(BF)
        cnt = _dot(rm.astype(BF), gsel)
        flag_ref[0] = jnp.max(cnt).astype(I32)

    flags()
    tk = mt_ref[0:8]
    gts = (mt_ref[8:16], mt_ref[16:24], mt_ref[24:32])
    blk1 = lax.broadcasted_iota(I32, (1, NT), 1) // 16
    ti = lax.broadcasted_iota(I32, (NT, NT), 0)
    tj = lax.broadcasted_iota(I32, (NT, NT), 1)
    earlier = ti < tj
    fc[...] = jnp.where(earlier & ((ti // 16) % 8 == (tj // 16) % 8), 1.0, 0.0).astype(BF)

    def rowmatch(r):
        lo = (r * 16).astype(F32)
        return jnp.max(jnp.where((tk >= lo) & (tk < lo + 16.0), 1.0, 0.0), axis=0, keepdims=True)
    rm = jnp.concatenate([rowmatch(iy), rowmatch(z * 2 + (1 - y)), jnp.zeros((6, NT), F32)], axis=0)
    rb = _dot(rm.astype(BF), fc[...])
    rb = rb - win_ref[0].astype(F32) * capc
    ridx = jnp.where((rm > 0.5) & (rb > -0.5) & (rb < capc - 0.5), rb, -1.0)
    gidx = ((blk1 % 2) * 2 + (blk1 // 2) % 2) * 2 + (blk1 // 4) % 2
    mine = gidx == (k * 2 + x) * 2 + y
    sj = lax.broadcasted_iota(I32, (NT, 64), 1)
    st = lax.broadcasted_iota(I32, (NT, 64), 0)
    sel = (st == (sj // 16) * 128 + y * 64 + ix * 16 + sj % 16).astype(F32).astype(BF)

    def mylist(n):
        ci = lax.broadcasted_iota(I32, (n, NT), 0).astype(F32)
        own = jnp.concatenate([(ci == jnp.where(mine, ridx[i:i + 1], -1.0)).astype(F32) for i in range(2)], axis=0)
        return _dot(own.astype(BF), sel).astype(BF)
    emat = mylist(cap)
    ematc = mylist(capc) if capc != cap else emat

    yc, xc, kc = {}, {}, {}

    def ystep(c):
        for cp in zc[c]:
            cp.wait_recv()
        lst = _dot(emat, zb[c].reshape(64, CW)).astype(BF)
        yb[c] = lst[cap:]
        yc[c] = _rcopy(yb.at[c], uc.at[c, k, x, y], ags.at[c, 3], agr.at[c, 3], p.ydev)
        yc[c].start()
        uc[c, k, x, y] = lst[:cap]

    def xstep(c):
        yc[c].wait_recv()
        xc[c] = _rcopy(uc.at[c, k, x], uc.at[c, k, x], ags.at[c, 4], agr.at[c, 4], p.xdev)
        xc[c].start()

    def kstep(c):
        xc[c].wait_recv()
        kc[c] = _rcopy(uc.at[c, k], uc.at[c, k], ags.at[c, 5], agr.at[c, 5], p.kdev)
        kc[c].start()

    for c in range(NC):
        ystep(c)
    xstep(0)

    scp[0].wait()
    u = u_ref[...]
    g = _dot(u, g1b[:, 6 * FF:7 * FF])
    xstep(1)
    scp[1].wait()
    v = _dot(u, g1b[:, 7 * FF:8 * FF])
    zs = (jax.nn.silu(g) * v).astype(BF)
    for i in range(2):
        wcp(3, i).start()
    xstep(2)

    fc[...] = jnp.where(earlier & (ti // 16 == tj // 16), 1.0, 0.0).astype(BF)
    ms, gs = [], []
    for e in range(4):
        eq = tk == (dev * 4 + e).astype(F32)
        ms.append(jnp.sum(jnp.where(eq, 1.0, 0.0), axis=0, keepdims=True))
        gs.append([jnp.sum(jnp.where(eq, gg, 0.0), axis=0, keepdims=True) for gg in gts])
    mstack = jnp.concatenate(ms + [jnp.zeros((4, NT), F32)], axis=0)
    before = _dot(mstack.astype(BF), fc[...])
    slot = jnp.where((mstack > 0.5) & (before < CAPE - 0.5), (blk1 * CAPE).astype(F32) + before, -1.0)
    def allists(n):
        cidx = jnp.where(ridx[0:1] > -0.5, (gidx * n).astype(F32) + ridx[0:1], -1.0)
        return (lax.broadcasted_iota(I32, (8 * n, NT), 0).astype(F32) == cidx).astype(F32).astype(BF)
    cmat = allists(cap)
    cmatc = allists(capc) if capc != cap else cmat
    si = lax.broadcasted_iota(I32, (128, NT), 0).astype(F32)
    xstep(3)
    for e in range(4):
        if e > 1:
            kstep(e - 2)
        hit = si == slot[e:e + 1]
        pm[128 * e:128 * (e + 1), :] = _dot_tt(hit.astype(F32).astype(BF), cmat).astype(BF)
        for m in range(3):
            gp = jnp.where(hit, gs[e][m], 0.0).astype(BF)
            gm[m, :, 128 * e:128 * (e + 1)] = _dot_tt(cmatc, gp).astype(BF)
    kstep(2)
    scp[2].wait()
    full = base[...] + _dot(zs, g2b[4 * FF:5 * FF, :]).astype(BF).astype(F32)
    base[...] = jnp.where(win_ref[0] == 0, full, 0.0)
    kstep(3)
    for c in range(NC):
        kc[c].wait_recv()
        xe[:, :, c * CW:(c + 1) * CW] = _dot(pm[...], uc[c].reshape(8 * cap, CW)).astype(BF).reshape(4, 128, CW)

    def ffn(e, _):
        wcp(e, 0).wait()
        g = _dot(xe[e], g1b[:, col13(e, 0)])
        wcp(e, 1).wait()
        v = _dot(xe[e], g1b[:, col13(e, 1)])
        zz[e] = (jax.nn.silu(g) * v).astype(BF)
        return 0
    lax.fori_loop(0, 4, ffn, 0)
    for e in range(4):
        wcp(e, 2).wait()

    ca, cx, cy, cz = {}, {}, {}, {}

    def stage0(c):
        for e in range(4):
            fc[128 * e:128 * (e + 1), :CX] = _dot(zz[e], g2b[FF * e:FF * (e + 1), c * CX:(c + 1) * CX]).astype(BF)
        f = fc[:, :CX]
        o = _dot(gm[0], f) + _dot(gm[1], f) + _dot(gm[2], f)
        ps[c] = o.reshape(2, 2, 2, capc, CX)
        ca[c] = _rcopy(ps.at[c, 1 - k], ra.at[c], cbs.at[c, 0], cbr.at[c, 0], p.kdev)
        ca[c].start()

    def stage1(c):
        ca[c].wait_recv()
        ps[c, k] = ps[c, k] + ra[c]
        cx[c] = _rcopy(ps.at[c, k, 1 - x], rx.at[c], cbs.at[c, 1], cbr.at[c, 1], p.xdev)
        cx[c].start()

    def stage2(c):
        cx[c].wait_recv()
        ps[c, k, x] = ps[c, k, x] + rx[c]
        cy[c] = _rcopy(ps.at[c, k, x, 1 - y], ry.at[c], cbs.at[c, 2], cbr.at[c, 2], p.ydev)
        cy[c].start()

    def stage3(c):
        cy[c].wait_recv()
        data = jnp.concatenate([ps[c, k, x, y], ry[c]], axis=0)
        a, b, d = _split3(data)
        dn = _dot_00(ematc, a) + _dot_00(ematc, b) + _dot_00(ematc, d)
        dz_buf[c] = dn.reshape(4, 16, CX)
        cz[c] = [_rcopy(dz_buf.at[c, (z + d) % 4], rz.at[c, d - 1], cbs.at[c, 2 + d], cbr.at[c, 2 + d], p.zdev(d))
                 for d in (1, 2, 3)]
        for cp in cz[c]:
            cp.start()

    def stage4(c):
        for cp in cz[c]:
            cp.wait_recv()
        o = base[:, c * CX:(c + 1) * CX] + dz_buf[c, z] + rz[c, 0] + rz[c, 1] + rz[c, 2]
        out_ref[:, c * CX:(c + 1) * CX] = o

    stages = (stage0, stage1, stage2, stage3, stage4)
    due = [0, 2, 6.6, 10.8, 17]
    for _, n, c in sorted((due[n] + c * (2.7 if n else 1.5), n, c) for n in range(5) for c in range(CC)):
        stages[n](c)
    for c in range(NC):
        for cp in zc[c] + [yc[c], xc[c], kc[c]]:
            cp.wait_send()
    for cp in m1 + m2:
        cp.wait_send()
    for c in range(CC):
        for cp in [ca[c], cx[c], cy[c]] + cz[c]:
            cp.wait_send()


def _layer(cap, capc, win, x, topk, gates, lens, ln1, ln2, *big):
    vm = pl.BlockSpec(memory_space=pltpu.VMEM)
    sm = pl.BlockSpec(memory_space=pltpu.SMEM)
    hb = pl.BlockSpec(memory_space=pl.ANY)
    dma = pltpu.SemaphoreType.DMA
    scratch = [
        pltpu.VMEM((16, D), BF), pltpu.VMEM((8, 16), I32), pltpu.VMEM((8, 16), F32), pltpu.VMEM((D,), BF), pltpu.VMEM((D,), BF),
        pltpu.VMEM((D, 8 * FF), BF), pltpu.VMEM((4096, D), BF),
        pltpu.VMEM((16, 1024, 128), BF), pltpu.VMEM((16, 1024, 128), BF),
        pltpu.VMEM((512, 128), F32), pltpu.VMEM((512, 128), F32), pltpu.VMEM((4, 2, 2, 2, 16, MW), BF),
        pltpu.VMEM((128, 128), F32), pltpu.VMEM((32, NT), F32), pltpu.VMEM((16, D), BF),
        pltpu.VMEM((NC, 4, 16, CW), BF), pltpu.VMEM((NC, cap, CW), BF), pltpu.VMEM((NC, 2, 2, 2, cap, CW), BF),
        pltpu.VMEM((4, 128, D), BF), pltpu.VMEM((4, 128, FF), BF), pltpu.VMEM((512, 512), BF),
        pltpu.VMEM((3, 8 * capc, 512), BF), pltpu.VMEM((512, 8 * cap), BF),
        pltpu.VMEM((CC, 2, 2, 2, capc, CX), F32), pltpu.VMEM((CC, 2, 2, capc, CX), F32),
        pltpu.VMEM((CC, 2, capc, CX), F32), pltpu.VMEM((CC, capc, CX), F32),
        pltpu.VMEM((CC, 4, 16, CX), F32), pltpu.VMEM((CC, 3, 16, CX), F32), pltpu.VMEM((16, D), F32),
        dma((5,)), dma((8,)), dma((8,)), dma((4,)), dma((4,)), dma((5, 3)), dma((10,)), dma((10,)),
        dma((NC, 6)), dma((NC, 6)), dma((CC, 6)), dma((CC, 6)),
    ]
    return pl.pallas_call(
        functools.partial(_layer_kernel, cap, capc),
        out_shape=(jax.ShapeDtypeStruct((16, D), F32), jax.ShapeDtypeStruct((1,), I32)),
        in_specs=[sm, sm] + [hb] * 15,
        out_specs=(vm, sm),
        scratch_shapes=scratch,
        name='layer',
        compiler_params=pltpu.CompilerParams(collective_id=1, has_side_effects=True, vmem_limit_bytes=67_043_328),
    )(jnp.full((1,), win, I32), lens, x, topk, gates, ln1, ln2, *big)


CAPD = 32
CAPC = 24


def solution(mesh):
    rows = P(('ey', 'ex'))
    rep = P()

    def local(x, kv_k, kv_v, lens, topk_idx, gates, ln1, ln2, wq, wo, ws1, ws3, ws2, w1, w3, w2):
        args = (x, topk_idx.T, gates.T, lens, ln1, ln2, wq, wo, kv_k.reshape(16, 1024, 128), kv_v.reshape(16, 1024, 128),
                ws1, ws3, ws2, w1, w3, w2)
        acc, most = _layer(CAPD, CAPC, 0, *args)

        def more(acc, args):
            for win in range(1, -(-64 // CAPC)):
                acc += _layer(CAPD, CAPC, win, *args)[0]
            return acc
        return lax.cond(most[0] > CAPC, more, lambda acc, _: acc, acc, args).astype(BF)

    return jax.shard_map(
        local, mesh=mesh,
        in_specs=(rows, rows, rows, rows, rows, rows, rep, rep, rep, rep, rep, rep, rep, rows, rows, rows),
        out_specs=rows, check_vma=False)
```

```python
import functools

import jax
import jax.numpy as jnp
from jax import lax
from jax.experimental import pallas as pl
from jax.experimental.pallas import tpu as pltpu
from jax.sharding import PartitionSpec as P

EPS = 1e-6
BF = jnp.bfloat16
F32 = jnp.float32
I32 = jnp.int32

D = 2048
FF = 768
NT = 512
CAPE = 4
NC = 4
CW = D // NC
CC = 4
CX = D // CC
MW = 128


def _rms(v, w):
    v = v.astype(F32)
    r = lax.rsqrt(jnp.mean(v * v, axis=-1, keepdims=True) + EPS)
    return (v * r * w.astype(F32)).astype(BF)


def _split3(v):
    a = v.astype(BF)
    r = v - a.astype(F32)
    b = r.astype(BF)
    c = (r - b.astype(F32)).astype(BF)
    return a, b, c


def _dot(a, b):
    return jnp.dot(a, b, preferred_element_type=F32)


def _dot_tt(a, b):
    return lax.dot_general(a, b, (((1,), (1,)), ((), ())), preferred_element_type=F32)


def _dot_00(a, b):
    return lax.dot_general(a, b, (((0,), (0,)), ((), ())), preferred_element_type=F32)


def _rcopy(src, dst, s, r, d):
    return pltpu.make_async_remote_copy(src_ref=src, dst_ref=dst, send_sem=s, recv_sem=r,
                                        device_id=d, device_id_type=pl.DeviceIdType.MESH)


class _Pos:
    def __init__(self):
        self.iy = iy = lax.axis_index('ey')
        self.ix = ix = lax.axis_index('ex')
        self.z, self.y = iy // 2, iy % 2
        self.x, self.k = ix // 2, ix % 2
        self.ydev = (self.z * 2 + (1 - self.y), ix)
        self.xdev = (iy, (1 - self.x) * 2 + self.k)
        self.kdev = (iy, self.x * 2 + (1 - self.k))

    def zdev(self, d):
        return (((self.z + d) % 4) * 2 + self.y, self.ix)

    def far(self, d):
        return (((self.z + d) % 4) * 2 + 1 - self.y, self.ix)

    def greet(self):
        barrier = pltpu.get_barrier_semaphore()
        for d in self.column() + self.row():
            pl.semaphore_signal(barrier, inc=1, device_id=d, device_id_type=pl.DeviceIdType.MESH)
        return barrier

    def column(self):
        return [self.zdev(d) for d in range(1, 4)] + [self.far(d) for d in range(4)]

    def row(self):
        return [(self.iy, (self.ix + d) % 4) for d in range(1, 4)]


def _layer_kernel(cap, capc, win_ref, lens_ref, x_hbm, topk_hbm, gates_hbm, ln1_hbm, ln2_hbm,
                  wq, wo, kk, vv, ws1, ws3, ws2, w1, w3, w2, out_ref, flag_ref,
                  x_ref, topk_ref, gates_ref, ln1_ref, ln2_ref, g1b, g2b, kb, vb, qs, os_, mall, mscr, mt_ref, u_ref,
                  zb, yb, uc, xe, zz, fc, gm, pm, ps, ra, rx, ry, dz_buf, rz, base,
                  isem, qsem, osem, ksem, vsem, esem, mgs, mgr, ags, agr, cbs, cbr):
    p = _Pos()
    iy, ix, z, y, x, k = p.iy, p.ix, p.z, p.y, p.x, p.k
    dev = iy * 4 + ix
    small = [pltpu.make_async_copy(s, d, isem.at[i]) for i, (s, d) in enumerate((
        (x_hbm, x_ref), (topk_hbm, topk_ref), (gates_hbm, gates_ref), (ln1_hbm, ln1_ref), (ln2_hbm, ln2_ref)))]
    for cp in small:
        cp.start()
    barrier = p.greet()

    def qcp(c):
        sl = pl.ds(pl.multiple_of(c * 512, 512), 512)
        return pltpu.make_async_copy(wq.at[:, sl], g1b.at[:, sl], qsem.at[c])

    def ocp(c):
        sl = pl.ds(pl.multiple_of(c * 512, 512), 512)
        return pltpu.make_async_copy(wo.at[sl], g2b.at[sl], osem.at[c])

    def kcp(t):
        return pltpu.make_async_copy(kk.at[pl.ds(t * 4, 4)], kb.at[pl.ds(t * 4, 4)], ksem.at[t])

    def vcp(t):
        return pltpu.make_async_copy(vv.at[pl.ds(t * 4, 4)], vb.at[pl.ds(t * 4, 4)], vsem.at[t])

    def col13(e, i):
        return pl.ds(pl.multiple_of((2 * e + i) * FF, 256), FF)

    def wcp(e, i):
        if i == 2:
            return pltpu.make_async_copy(w2.at[e], g2b.at[pl.ds(pl.multiple_of(e * FF, 256), FF)], esem.at[e, 2])
        return pltpu.make_async_copy((w1, w3)[i].at[e], g1b.at[:, col13(e, i)], esem.at[e, i])
    scp = [pltpu.make_async_copy(ws1, g1b.at[:, col13(3, 0)], esem.at[4, 0]),
           pltpu.make_async_copy(ws3, g1b.at[:, col13(3, 1)], esem.at[4, 1]),
           pltpu.make_async_copy(ws2, g2b.at[pl.ds(4 * FF, FF)], esem.at[4, 2])]

    for c in range(8):
        qcp(c).start()
    for t in range(4):
        kcp(t).start()
        vcp(t).start()
    for c in range(8):
        ocp(c).start()
    scp[0].start()
    scp[1].start()

    for cp in small:
        cp.wait()
    mscr[...] = jnp.zeros((128, 128), F32)
    mscr[0:8, 0:16] = topk_ref[...].astype(F32)
    for i, part in enumerate(_split3(gates_ref[...])):
        mscr[8 + 8 * i:16 + 8 * i, 0:16] = part.astype(F32)
    mall[z, y, x, k] = mscr[...].T[0:16].astype(BF)
    a = _rms(x_ref[...], ln1_ref[...].reshape(1, D))

    own = mall.at[z, y, x, k]
    m1 = [_rcopy(own, own, mgs.at[i], mgr.at[i], d) for i, d in enumerate(p.column())]
    col = mall.at[:, :, x, k]
    m2 = [_rcopy(col, col, mgs.at[7 + i], mgr.at[7 + i], d) for i, d in enumerate(p.row())]

    def qstep(c, _):
        @pl.when(c == 5)
        def _():
            pl.semaphore_wait(barrier, 10)
            for cp in m1:
                cp.start()
        qcp(c).wait()
        q = _dot(a, g1b[:, pl.ds(pl.multiple_of(c * 512, 512), 512)]).astype(BF).astype(F32)
        for j in range(4):
            qs[pl.ds(pl.multiple_of(c * 64 + j * 16, 16), 16), :] = q[:, j * 128:(j + 1) * 128]
        return 0
    lax.fori_loop(0, 8, qstep, 0)
    for e in range(3):
        wcp(e, 0).start()
        wcp(e, 1).start()

    col = lax.broadcasted_iota(I32, (64, 1024), 1)
    row = lax.broadcasted_iota(I32, (64, 1024), 0)
    pos = jnp.where((col % 4) == (row % 32) // 8, col // 4, 1 << 20)
    first = lax.broadcasted_iota(I32, (64, 1), 0) < 32
    nil = jnp.zeros((32, 128), BF)

    def astep(g, _):
        @pl.when(g == 2)
        def _():
            for cp in m1:
                cp.wait_recv()
            for cp in m2:
                cp.start()
        kcp(g).wait()
        vcp(g).wait()
        for j in range(2):
            t = g * 4 + 2 * j
            qa = qs[pl.ds(t, 32, stride=16), :].astype(BF)
            qb = qs[pl.ds(t + 1, 32, stride=16), :].astype(BF)
            q2 = jnp.concatenate([jnp.concatenate([qa, nil], axis=1), jnp.concatenate([nil, qb], axis=1)], axis=0)
            s = _dot_tt(q2, jnp.concatenate([kb[t], kb[t + 1]], axis=1))
            s = jnp.where(pos < jnp.where(first, lens_ref[t], lens_ref[t + 1]), s, -jnp.inf)
            m = jnp.max(s, axis=1, keepdims=True)
            e = jnp.exp((s - m) * 128.0 ** -0.5)
            pr = (e * (1.0 / jnp.sum(e, axis=1, keepdims=True))).astype(BF)
            o = _dot(pr, jnp.concatenate([vb[t], vb[t + 1]], axis=1))
            os_[pl.ds(t, 32, stride=16), :] = o[:32, :128]
            os_[pl.ds(t + 1, 32, stride=16), :] = o[32:, 128:]
        return 0
    lax.fori_loop(0, 4, astep, 0)

    base[...] = x_ref[...].astype(F32)

    def ostep(c, _):
        ocp(c).wait()
        oc = jnp.concatenate([os_[pl.ds(pl.multiple_of(c * 64 + j * 16, 16), 16), :] for j in range(4)], axis=1).astype(BF)
        base[...] += _dot(oc, g2b[pl.ds(pl.multiple_of(c * 512, 512), 512), :])
        return 0
    lax.fori_loop(0, 8, ostep, 0)
    h = base[...].astype(BF)
    u_ref[...] = _rms(h, ln2_ref[...].reshape(1, D))
    base[...] = h.astype(F32)

    zc = []
    for c in range(NC):
        zb[c, z] = u_ref[:, CW * c:CW * (c + 1)]
    for c in range(NC):
        blk = zb.at[c, z]
        cps = [_rcopy(blk, blk, ags.at[c, d - 1], agr.at[c, d - 1], p.zdev(d)) for d in (2, 1, 3)]
        for cp in cps:
            cp.start()
        zc.append(cps)
    scp[2].start()
    for e in range(4):
        wcp(e, 2).start()

    for cp in m2:
        cp.wait_recv()
    def flags():
        mt = mall[...].reshape(NT, MW).astype(F32).T[0:32]
        mt_ref[...] = mt
        tk = mt[0:8]
        rm = jnp.concatenate([jnp.max(jnp.where((tk >= 16.0 * r) & (tk < 16.0 * r + 16.0), 1.0, 0.0), axis=0, keepdims=True)
                              for r in range(8)], axis=0)
        gt = (lax.broadcasted_iota(I32, (NT, 128), 0) // 16) % 8
        gsel = (gt == lax.broadcasted_iota(I32, (NT, 128), 1)).astype(F32).astype(BF)
        cnt = _dot(rm.astype(BF), gsel)
        flag_ref[0] = jnp.max(cnt).astype(I32)

    flags()
    tk = mt_ref[0:8]
    gts = (mt_ref[8:16], mt_ref[16:24], mt_ref[24:32])
    blk1 = lax.broadcasted_iota(I32, (1, NT), 1) // 16
    ti = lax.broadcasted_iota(I32, (NT, NT), 0)
    tj = lax.broadcasted_iota(I32, (NT, NT), 1)
    earlier = ti < tj
    fc[...] = jnp.where(earlier & ((ti // 16) % 8 == (tj // 16) % 8), 1.0, 0.0).astype(BF)

    def rowmatch(r):
        lo = (r * 16).astype(F32)
        return jnp.max(jnp.where((tk >= lo) & (tk < lo + 16.0), 1.0, 0.0), axis=0, keepdims=True)
    rm = jnp.concatenate([rowmatch(iy), rowmatch(z * 2 + (1 - y)), jnp.zeros((6, NT), F32)], axis=0)
    rb = _dot(rm.astype(BF), fc[...])
    rb = rb - win_ref[0].astype(F32) * capc
    ridx = jnp.where((rm > 0.5) & (rb > -0.5) & (rb < capc - 0.5), rb, -1.0)
    gidx = ((blk1 % 2) * 2 + (blk1 // 2) % 2) * 2 + (blk1 // 4) % 2
    mine = gidx == (k * 2 + x) * 2 + y
    sj = lax.broadcasted_iota(I32, (NT, 64), 1)
    st = lax.broadcasted_iota(I32, (NT, 64), 0)
    sel = (st == (sj // 16) * 128 + y * 64 + ix * 16 + sj % 16).astype(F32).astype(BF)

    def mylist(n):
        ci = lax.broadcasted_iota(I32, (n, NT), 0).astype(F32)
        own = jnp.concatenate([(ci == jnp.where(mine, ridx[i:i + 1], -1.0)).astype(F32) for i in range(2)], axis=0)
        return _dot(own.astype(BF), sel).astype(BF)
    emat = mylist(cap)
    ematc = mylist(capc) if capc != cap else emat

    yc, xc, kc = {}, {}, {}

    def ystep(c):
        for cp in zc[c]:
            cp.wait_recv()
        lst = _dot(emat, zb[c].reshape(64, CW)).astype(BF)
        yb[c] = lst[cap:]
        yc[c] = _rcopy(yb.at[c], uc.at[c, k, x, y], ags.at[c, 3], agr.at[c, 3], p.ydev)
        yc[c].start()
        uc[c, k, x, y] = lst[:cap]

    def xstep(c):
        yc[c].wait_recv()
        xc[c] = _rcopy(uc.at[c, k, x], uc.at[c, k, x], ags.at[c, 4], agr.at[c, 4], p.xdev)
        xc[c].start()

    def kstep(c):
        xc[c].wait_recv()
        kc[c] = _rcopy(uc.at[c, k], uc.at[c, k], ags.at[c, 5], agr.at[c, 5], p.kdev)
        kc[c].start()

    for c in range(NC):
        ystep(c)
    xstep(0)

    scp[0].wait()
    u = u_ref[...]
    g = _dot(u, g1b[:, 6 * FF:7 * FF])
    xstep(1)
    scp[1].wait()
    v = _dot(u, g1b[:, 7 * FF:8 * FF])
    zs = (jax.nn.silu(g) * v).astype(BF)
    for i in range(2):
        wcp(3, i).start()
    xstep(2)

    fc[...] = jnp.where(earlier & (ti // 16 == tj // 16), 1.0, 0.0).astype(BF)
    ms, gs = [], []
    for e in range(4):
        eq = tk == (dev * 4 + e).astype(F32)
        ms.append(jnp.sum(jnp.where(eq, 1.0, 0.0), axis=0, keepdims=True))
        gs.append([jnp.sum(jnp.where(eq, gg, 0.0), axis=0, keepdims=True) for gg in gts])
    mstack = jnp.concatenate(ms + [jnp.zeros((4, NT), F32)], axis=0)
    before = _dot(mstack.astype(BF), fc[...])
    slot = jnp.where((mstack > 0.5) & (before < CAPE - 0.5), (blk1 * CAPE).astype(F32) + before, -1.0)
    def allists(n):
        cidx = jnp.where(ridx[0:1] > -0.5, (gidx * n).astype(F32) + ridx[0:1], -1.0)
        return (lax.broadcasted_iota(I32, (8 * n, NT), 0).astype(F32) == cidx).astype(F32).astype(BF)
    cmat = allists(cap)
    cmatc = allists(capc) if capc != cap else cmat
    si = lax.broadcasted_iota(I32, (128, NT), 0).astype(F32)
    xstep(3)
    for e in range(4):
        if e > 1:
            kstep(e - 2)
        hit = si == slot[e:e + 1]
        pm[128 * e:128 * (e + 1), :] = _dot_tt(hit.astype(F32).astype(BF), cmat).astype(BF)
        for m in range(3):
            gp = jnp.where(hit, gs[e][m], 0.0).astype(BF)
            gm[m, :, 128 * e:128 * (e + 1)] = _dot_tt(cmatc, gp).astype(BF)
    kstep(2)
    scp[2].wait()
    full = base[...] + _dot(zs, g2b[4 * FF:5 * FF, :]).astype(BF).astype(F32)
    base[...] = jnp.where(win_ref[0] == 0, full, 0.0)
    kstep(3)
    for c in range(NC):
        kc[c].wait_recv()
        xe[:, :, c * CW:(c + 1) * CW] = _dot(pm[...], uc[c].reshape(8 * cap, CW)).astype(BF).reshape(4, 128, CW)

    def ffn(e, _):
        wcp(e, 0).wait()
        g = _dot(xe[e], g1b[:, col13(e, 0)])
        wcp(e, 1).wait()
        v = _dot(xe[e], g1b[:, col13(e, 1)])
        zz[e] = (jax.nn.silu(g) * v).astype(BF)
        return 0
    lax.fori_loop(0, 4, ffn, 0)
    for e in range(4):
        wcp(e, 2).wait()

    ca, cx, cy, cz = {}, {}, {}, {}

    def stage0(c):
        for e in range(4):
            fc[128 * e:128 * (e + 1), :CX] = _dot(zz[e], g2b[FF * e:FF * (e + 1), c * CX:(c + 1) * CX]).astype(BF)
        f = fc[:, :CX]
        o = _dot(gm[0], f) + _dot(gm[1], f) + _dot(gm[2], f)
        ps[c] = o.reshape(2, 2, 2, capc, CX)
        ca[c] = _rcopy(ps.at[c, 1 - k], ra.at[c], cbs.at[c, 0], cbr.at[c, 0], p.kdev)
        ca[c].start()

    def stage1(c):
        ca[c].wait_recv()
        ps[c, k] = ps[c, k] + ra[c]
        cx[c] = _rcopy(ps.at[c, k, 1 - x], rx.at[c], cbs.at[c, 1], cbr.at[c, 1], p.xdev)
        cx[c].start()

    def stage2(c):
        cx[c].wait_recv()
        ps[c, k, x] = ps[c, k, x] + rx[c]
        cy[c] = _rcopy(ps.at[c, k, x, 1 - y], ry.at[c], cbs.at[c, 2], cbr.at[c, 2], p.ydev)
        cy[c].start()

    def stage3(c):
        cy[c].wait_recv()
        data = jnp.concatenate([ps[c, k, x, y], ry[c]], axis=0)
        a, b, d = _split3(data)
        dn = _dot_00(ematc, a) + _dot_00(ematc, b) + _dot_00(ematc, d)
        dz_buf[c] = dn.reshape(4, 16, CX)
        cz[c] = [_rcopy(dz_buf.at[c, (z + d) % 4], rz.at[c, d - 1], cbs.at[c, 2 + d], cbr.at[c, 2 + d], p.zdev(d))
                 for d in (2, 1, 3)]
        for cp in cz[c]:
            cp.start()

    def stage4(c):
        for cp in cz[c]:
            cp.wait_recv()
        o = base[:, c * CX:(c + 1) * CX] + dz_buf[c, z] + rz[c, 0] + rz[c, 1] + rz[c, 2]
        out_ref[:, c * CX:(c + 1) * CX] = o

    stages = (stage0, stage1, stage2, stage3, stage4)
    due = [0, 2, 6.6, 10.8, 17]
    for _, n, c in sorted((due[n] + c * (2.7 if n else 1.5), n, c) for n in range(5) for c in range(CC)):
        stages[n](c)
    for c in range(NC):
        for cp in zc[c] + [yc[c], xc[c], kc[c]]:
            cp.wait_send()
    for cp in m1 + m2:
        cp.wait_send()
    for c in range(CC):
        for cp in [ca[c], cx[c], cy[c]] + cz[c]:
            cp.wait_send()


def _layer(cap, capc, win, x, topk, gates, lens, ln1, ln2, *big):
    vm = pl.BlockSpec(memory_space=pltpu.VMEM)
    sm = pl.BlockSpec(memory_space=pltpu.SMEM)
    hb = pl.BlockSpec(memory_space=pl.ANY)
    dma = pltpu.SemaphoreType.DMA
    scratch = [
        pltpu.VMEM((16, D), BF), pltpu.VMEM((8, 16), I32), pltpu.VMEM((8, 16), F32), pltpu.VMEM((D,), BF), pltpu.VMEM((D,), BF),
        pltpu.VMEM((D, 8 * FF), BF), pltpu.VMEM((4096, D), BF),
        pltpu.VMEM((16, 1024, 128), BF), pltpu.VMEM((16, 1024, 128), BF),
        pltpu.VMEM((512, 128), F32), pltpu.VMEM((512, 128), F32), pltpu.VMEM((4, 2, 2, 2, 16, MW), BF),
        pltpu.VMEM((128, 128), F32), pltpu.VMEM((32, NT), F32), pltpu.VMEM((16, D), BF),
        pltpu.VMEM((NC, 4, 16, CW), BF), pltpu.VMEM((NC, cap, CW), BF), pltpu.VMEM((NC, 2, 2, 2, cap, CW), BF),
        pltpu.VMEM((4, 128, D), BF), pltpu.VMEM((4, 128, FF), BF), pltpu.VMEM((512, 512), BF),
        pltpu.VMEM((3, 8 * capc, 512), BF), pltpu.VMEM((512, 8 * cap), BF),
        pltpu.VMEM((CC, 2, 2, 2, capc, CX), F32), pltpu.VMEM((CC, 2, 2, capc, CX), F32),
        pltpu.VMEM((CC, 2, capc, CX), F32), pltpu.VMEM((CC, capc, CX), F32),
        pltpu.VMEM((CC, 4, 16, CX), F32), pltpu.VMEM((CC, 3, 16, CX), F32), pltpu.VMEM((16, D), F32),
        dma((5,)), dma((8,)), dma((8,)), dma((4,)), dma((4,)), dma((5, 3)), dma((10,)), dma((10,)),
        dma((NC, 6)), dma((NC, 6)), dma((CC, 6)), dma((CC, 6)),
    ]
    return pl.pallas_call(
        functools.partial(_layer_kernel, cap, capc),
        out_shape=(jax.ShapeDtypeStruct((16, D), F32), jax.ShapeDtypeStruct((1,), I32)),
        in_specs=[sm, sm] + [hb] * 15,
        out_specs=(vm, sm),
        scratch_shapes=scratch,
        name='layer',
        compiler_params=pltpu.CompilerParams(collective_id=1, has_side_effects=True, vmem_limit_bytes=67_043_328),
    )(jnp.full((1,), win, I32), lens, x, topk, gates, ln1, ln2, *big)


CAPD = 32
CAPC = 24


def solution(mesh):
    rows = P(('ey', 'ex'))
    rep = P()

    def local(x, kv_k, kv_v, lens, topk_idx, gates, ln1, ln2, wq, wo, ws1, ws3, ws2, w1, w3, w2):
        args = (x, topk_idx.T, gates.T, lens, ln1, ln2, wq, wo, kv_k.reshape(16, 1024, 128), kv_v.reshape(16, 1024, 128),
                ws1, ws3, ws2, w1, w3, w2)
        acc, most = _layer(CAPD, CAPC, 0, *args)

        def more(acc, args):
            for win in range(1, -(-64 // CAPC)):
                acc += _layer(CAPD, CAPC, win, *args)[0]
            return acc
        return lax.cond(most[0] > CAPC, more, lambda acc, _: acc, acc, args).astype(BF)

    return jax.shard_map(
        local, mesh=mesh,
        in_specs=(rows, rows, rows, rows, rows, rows, rep, rep, rep, rep, rep, rep, rep, rows, rows, rows),
        out_specs=rows, check_vma=False)
```
